16 devices in a mesh: dp: 2 (over z), ep: 8 (over y, x, core).
Axes of the slice: x: 2, y: 2, z: 2, core: 2. Of those that a mesh axis runs over, the one named last changes fastest.
Arguments:
- h0: bfloat16 [16, 256, 2048], P(('dp', 'ep')), parts along dimension 0
- idx: int32 [16, 256, 8], P(('dp', 'ep')), parts along dimension 0
- slot: int32 [16, 256, 8], P(('dp', 'ep')), parts along dimension 0
- norm_attn: bfloat16 [2048], replicated
- wq: bfloat16 [2048, 2048], replicated
- wk: bfloat16 [2048, 2048], replicated
- wv: bfloat16 [2048, 2048], replicated
- wo: bfloat16 [2048, 2048], replicated
- norm_ffn: bfloat16 [2048], replicated
- w1: bfloat16 [2048, 8192], replicated
- w3: bfloat16 [2048, 8192], replicated
- w2: bfloat16 [8192, 2048], replicated
- norm_moe: bfloat16 [2048], replicated
- wr: bfloat16 [2048, 64], replicated
- ue1: bfloat16 [64, 2048, 1024], P('ep')
- ue3: bfloat16 [64, 2048, 1024], P('ep')
- ue2: bfloat16 [64, 1024, 2048], P('ep')
Outputs:
- output: bfloat16 [16, 256, 2048], P(('dp', 'ep')), parts along dimension 0
There are 2 independent parts. The reference program is written for one: setup_inputs(seed, part) draws one part's arguments, and reference() takes and returns one part's arrays. A program takes and returns all parts, laid end to end along the dimension named above; an argument that names none is the same for every part.
All inputs are finite; a program needn't handle non-finite values.
Results may differ from the reference program's by a relative error of at most 0.0105677.
Values are sent between devices in bfloat16 or wider.
A program may use at most 1 GiB of HBM per device.

```python
import jax
import jax.numpy as jnp
from jax import lax

D = 2048
HEADS = 16
KV_HEADS = 16
HEAD = 128
FF = 8192
EXPERTS = 64
TOP = 8
FE = 1024
SEQS_DEV = 1
SEQ = 256
EP = 8

TOKENS = SEQS_DEV * SEQ
CAP = 2 * TOKENS * TOP // EXPERTS
EPS = 1e-6
ROPE_BASE = 10000.0


def _w(key, shape, fan_in, scale=1.0):
    return (scale * fan_in ** -0.5 * jax.random.normal(key, shape, jnp.float32)).astype(jnp.bfloat16)


def _perms(key, count, size):
    return jax.vmap(lambda k: jax.random.permutation(k, size))(jax.random.split(key, count))


def setup_inputs(seed: int = 0, part: int = 0) -> dict:
    key = jax.random.PRNGKey(seed)
    ks = jax.random.split(key, 14)
    kp = jax.random.split(jax.random.fold_in(key, part), 4)
    kd = jax.random.split(jax.random.fold_in(jax.random.fold_in(key, part), 7), 4)
    avg = TOKENS * TOP // EXPERTS
    c = jnp.arange(TOKENS * TOP).reshape(TOKENS, TOP)
    half = TOKENS * TOP // 2
    low = c < half
    e0 = jnp.where(low, c % EXPERTS, (c - half) % (EXPERTS // 2))
    s0 = jnp.where(low, c // EXPERTS, avg // 2 + (c - half) // (EXPERTS // 2))
    shift = jax.random.randint(kd[2], (EP, EXPERTS), 0, CAP)
    tperm = jnp.broadcast_to(_perms(kd[3], EP, TOKENS)[:, :, None], (EP, TOKENS, TOP))
    idx = jnp.take_along_axis(jnp.broadcast_to(e0, (EP, TOKENS, TOP)), tperm, axis=1)
    slot = jnp.take_along_axis((s0[None] + shift[:, e0]) % CAP, tperm, axis=1)
    rshape = (EP * SEQS_DEV, SEQ, TOP)

    def nrm(k):
        return (1.0 + 0.2 * jax.random.normal(k, (D,), jnp.float32)).astype(jnp.bfloat16)

    return {
        'h0': jax.random.normal(kp[0], (EP * SEQS_DEV, SEQ, D), jnp.float32).astype(jnp.bfloat16),
        'idx': idx.reshape(rshape).astype(jnp.int32),
        'slot': slot.reshape(rshape).astype(jnp.int32),
        'norm_attn': nrm(ks[0]),
        'wq': _w(ks[1], (D, HEADS * HEAD), D),
        'wk': _w(ks[2], (D, KV_HEADS * HEAD), D),
        'wv': _w(ks[3], (D, KV_HEADS * HEAD), D),
        'wo': _w(ks[4], (HEADS * HEAD, D), HEADS * HEAD, 2.0),
        'norm_ffn': nrm(ks[5]),
        'w1': _w(ks[6], (D, FF), D),
        'w3': _w(ks[7], (D, FF), D),
        'w2': _w(ks[8], (FF, D), FF, 2.0),
        'norm_moe': nrm(ks[9]),
        'wr': _w(ks[10], (D, EXPERTS), D, 2.0),
        'ue1': _w(ks[11], (EXPERTS, D, FE), D),
        'ue3': _w(ks[12], (EXPERTS, D, FE), D),
        'ue2': _w(ks[13], (EXPERTS, FE, D), FE, 2.0),
    }


def _rms(x, w):
    xf = x.astype(jnp.float32)
    r = lax.rsqrt(jnp.mean(xf * xf, axis=-1, keepdims=True) + EPS)
    return (xf * r * w.astype(jnp.float32)).astype(jnp.bfloat16)


def _rope(x, cos, sin):
    h = HEAD // 2
    x1 = x[..., :h]
    x2 = x[..., h:]
    return jnp.concatenate([x1 * cos - x2 * sin, x2 * cos + x1 * sin], axis=-1)


def _dense_seq(h, na, wq, wk, wv, wo, nf, w1, w3, w2):
    f32 = jnp.float32
    bf = jnp.bfloat16
    pos = jnp.arange(SEQ).astype(f32)
    inv = ROPE_BASE ** (-2.0 * jnp.arange(HEAD // 2).astype(f32) / HEAD)
    ang = pos[:, None] * inv[None, :]
    cos = jnp.cos(ang)[:, None, :]
    sin = jnp.sin(ang)[:, None, :]
    x = _rms(h, na)
    q = _rope(jnp.dot(x, wq, preferred_element_type=f32).reshape(SEQ, HEADS, HEAD), cos, sin).astype(bf)
    k = _rope(jnp.dot(x, wk, preferred_element_type=f32).reshape(SEQ, KV_HEADS, HEAD), cos, sin).astype(bf)
    v = jnp.dot(x, wv, preferred_element_type=f32).astype(bf).reshape(SEQ, KV_HEADS, HEAD)
    q = q.reshape(SEQ, KV_HEADS, HEADS // KV_HEADS, HEAD)
    s = jnp.einsum('qgrd,kgd->grqk', q.astype(f32), k.astype(f32)) * HEAD ** -0.5
    causal = jnp.arange(SEQ)[:, None] >= jnp.arange(SEQ)[None, :]
    s = jnp.where(causal, s, -jnp.inf)
    p = jax.nn.softmax(s, axis=-1).astype(bf)
    o = jnp.einsum('grqk,kgd->qgrd', p.astype(f32), v.astype(f32)).astype(bf).reshape(SEQ, HEADS * HEAD)
    a = (h.astype(f32) + jnp.dot(o, wo, preferred_element_type=f32)).astype(bf)
    z = _rms(a, nf)
    hid = (jax.nn.silu(jnp.dot(z, w1, preferred_element_type=f32)) * jnp.dot(z, w3, preferred_element_type=f32)).astype(bf)
    return a.astype(f32) + jnp.dot(hid, w2, preferred_element_type=f32)


def reference(h0, idx, slot, norm_attn, wq, wk, wv, wo, norm_ffn, w1, w3, w2, norm_moe, wr, ue1, ue3, ue2):
    f32 = jnp.float32
    bf = jnp.bfloat16
    n = EP * TOKENS
    ix = idx.reshape(n, TOP)
    sl = slot.reshape(n, TOP)
    u = _rms(h0.reshape(n, D), norm_moe)
    logits = jnp.dot(u, wr, preferred_element_type=f32)
    g = jax.nn.softmax(jnp.take_along_axis(logits, ix, axis=1), axis=-1)
    rows = jnp.broadcast_to(jnp.arange(n, dtype=jnp.int32)[:, None], (n, TOP))
    src = rows // TOKENS
    tok = jnp.full((EP, EXPERTS, CAP), n, jnp.int32).at[src, ix, sl].set(rows)
    gb = jnp.zeros((EP, EXPERTS, CAP), f32).at[src, ix, sl].set(g)
    tok = tok.transpose(1, 0, 2).reshape(EXPERTS, EP * CAP)
    x = jnp.take(u, tok, axis=0, mode='fill', fill_value=0)

    def expert(args):
        xe, e1, e3, e2 = args
        hid = (jax.nn.silu(jnp.dot(xe, e1, preferred_element_type=f32)) * jnp.dot(xe, e3, preferred_element_type=f32)).astype(bf)
        return jnp.dot(hid, e2, preferred_element_type=f32).astype(bf)

    y = lax.map(expert, (x, ue1, ue3, ue2))
    gw = gb.transpose(1, 0, 2).reshape(EXPERTS, EP * CAP, 1)
    m = jnp.zeros((n, D), f32).at[tok.reshape(-1)].add((gw * y.astype(f32)).reshape(-1, D), mode='drop')
    dense = lax.map(lambda hs: _dense_seq(hs, norm_attn, wq, wk, wv, wo, norm_ffn, w1, w3, w2), h0)
    return (dense + m.reshape(EP * SEQS_DEV, SEQ, D)).astype(bf)
```

```python
import functools

import jax
import jax.numpy as jnp
from jax import lax
from jax.experimental import pallas as pl
from jax.experimental.pallas import tpu as pltpu
from jax.sharding import PartitionSpec as P

HEAD = 128
EPS = 1e-6
ROPE_BASE = 10000.0
F32, BF = jnp.float32, jnp.bfloat16


def _rms(x, w):
    xf = x.astype(F32)
    r = lax.rsqrt(jnp.mean(xf * xf, axis=-1, keepdims=True) + EPS)
    return (xf * r * w.astype(F32)).astype(BF)


def _dot(a, b):
    return jnp.dot(a, b, preferred_element_type=F32)


def _attn_kernel(h_ref, na_ref, cos_ref, sin_ref, wq_ref, wk_ref, wv_ref, wo_ref, a_ref, x_sc, acc_sc, *, nsteps, hps):
    i = pl.program_id(0)
    t = h_ref.shape[0]

    @pl.when(i == 0)
    def _():
        x_sc[...] = _rms(h_ref[...], na_ref[...])
        acc_sc[...] = jnp.zeros_like(acc_sc)

    x = x_sc[...]
    q2 = _dot(x, wq_ref[...])
    k2 = _dot(x, wk_ref[...])
    v2 = _dot(x, wv_ref[...]).astype(BF)
    cos, sin = cos_ref[...], sin_ref[...]
    causal = lax.broadcasted_iota(jnp.int32, (t, t), 0) >= lax.broadcasted_iota(jnp.int32, (t, t), 1)
    outs = []
    for h in range(hps):
        sl = slice(h * HEAD, (h + 1) * HEAD)
        q, k, v = q2[:, sl], k2[:, sl], v2[:, sl]
        q = (q * cos + pltpu.roll(q, HEAD // 2, 1) * sin).astype(BF)
        k = (k * cos + pltpu.roll(k, HEAD // 2, 1) * sin).astype(BF)
        s = lax.dot_general(q, k, (((1,), (1,)), ((), ())), preferred_element_type=F32) * HEAD ** -0.5
        s = jnp.where(causal, s, -jnp.inf)
        p = jnp.exp(s - jnp.max(s, axis=-1, keepdims=True))
        p = (p / jnp.sum(p, axis=-1, keepdims=True)).astype(BF)
        outs.append(_dot(p, v).astype(BF))
    o = jnp.concatenate(outs, axis=1)
    acc_sc[...] += _dot(o, wo_ref[...])

    @pl.when(i == nsteps - 1)
    def _():
        a_ref[...] = (h_ref[...].astype(F32) + acc_sc[...]).astype(BF)


def _attention(h, na, wq, wk, wv, wo):
    t, d = h.shape
    hps = 2
    nsteps = wq.shape[1] // (HEAD * hps)
    w = HEAD * hps
    pos = jnp.arange(t).astype(F32)
    inv = ROPE_BASE ** (-2.0 * jnp.arange(HEAD // 2).astype(F32) / HEAD)
    ang = pos[:, None] * inv[None, :]
    c, s = jnp.cos(ang), jnp.sin(ang)
    cos, sin = jnp.concatenate([c, c], 1), jnp.concatenate([-s, s], 1)
    full = lambda shape: pl.BlockSpec(shape, lambda i: (0, 0))
    return pl.pallas_call(
        functools.partial(_attn_kernel, nsteps=nsteps, hps=hps),
        grid=(nsteps,),
        in_specs=[full((t, d)), full((1, d)), full((t, HEAD)), full((t, HEAD))]
        + [pl.BlockSpec((d, w), lambda i: (0, i))] * 3
        + [pl.BlockSpec((w, d), lambda i: (i, 0))],
        out_specs=full((t, d)),
        out_shape=jax.ShapeDtypeStruct((t, d), BF),
        scratch_shapes=[pltpu.VMEM((t, d), BF), pltpu.VMEM((t, d), F32)],
        cost_estimate=pl.CostEstimate(flops=8 * t * d * d, bytes_accessed=8 * d * d, transcendentals=0),
        compiler_params=pltpu.CompilerParams(dimension_semantics=("arbitrary",)),
        name="attn",
    )(h, na.reshape(1, d), cos, sin, wq, wk, wv, wo)


def _ffn_kernel(a_ref, nf_ref, w1_ref, w3_ref, w2_ref, o_ref, z_sc, *, nsteps):
    i = pl.program_id(0)

    @pl.when(i == 0)
    def _():
        z_sc[...] = _rms(a_ref[...], nf_ref[...])
        o_ref[...] = a_ref[...].astype(F32)

    z = z_sc[...]
    h1 = _dot(z, w1_ref[...])
    h3 = _dot(z, w3_ref[...])
    hid = (h1 * jax.nn.sigmoid(h1) * h3).astype(BF)
    o_ref[...] += _dot(hid, w2_ref[...])


def _ffn(a, nf, w1, w3, w2):
    t, d = a.shape
    ff = w1.shape[1]
    ft = 512
    nsteps = ff // ft
    full = lambda shape: pl.BlockSpec(shape, lambda i: (0, 0))
    return pl.pallas_call(
        functools.partial(_ffn_kernel, nsteps=nsteps),
        grid=(nsteps,),
        in_specs=[full((t, d)), full((1, d))]
        + [pl.BlockSpec((d, ft), lambda i: (0, i))] * 2
        + [pl.BlockSpec((ft, d), lambda i: (i, 0))],
        out_specs=full((t, d)),
        out_shape=jax.ShapeDtypeStruct((t, d), F32),
        scratch_shapes=[pltpu.VMEM((t, d), BF)],
        cost_estimate=pl.CostEstimate(flops=6 * t * d * ff, bytes_accessed=6 * d * ff, transcendentals=0),
        compiler_params=pltpu.CompilerParams(dimension_semantics=("arbitrary",)),
        name="ffn",
    )(a, nf.reshape(1, d), w1, w3, w2)


def _expert_kernel(off_ref, nb_ref, u_ref, rt_ref, r_ref, g_ref, w1_ref, w3_ref, w2_ref, o_ref,
                   x_sc, acc_sc, y_sc, *, ns, el, cap, nf, mb):
    i = pl.program_id(0)
    d = u_ref.shape[-1]
    t = u_ref.shape[1]
    rows = ns * cap

    @pl.when(i < ns)
    def _():
        it = lax.broadcasted_iota(jnp.int32, (cap, t), 0)
        p = jnp.concatenate(
            [jnp.where(it == rt_ref[0, e:e + 1, :], 1.0, 0.0).astype(BF) for e in range(el)], axis=0)
        for c in range(d // 512):
            cs = slice(c * 512, (c + 1) * 512)
            xv = _dot(p, u_ref[0, :, cs]).astype(BF)
            for e in range(el):
                o = pl.multiple_of(off_ref[i * el + e], 16)
                x_sc[e, pl.ds(o, cap), cs] = xv[e * cap:(e + 1) * cap]

    j = i - ns
    for m in range(mb, rows + 1, mb):
        e = lax.div(jnp.maximum(j, 0), nf)

        @pl.when((j >= 0) & (j < el * nf) & (nb_ref[jnp.minimum(e, el - 1)] == m // mb))
        def _():
            f = lax.rem(j, nf)
            x = x_sc[e, :m, :]
            h1 = _dot(x, w1_ref[0])
            h3 = _dot(x, w3_ref[0])
            hid = (h1 * jax.nn.sigmoid(h1) * h3).astype(BF)
            y = _dot(hid, w2_ref[0])

            @pl.when(f == 0)
            def _():
                acc_sc[:m, :] = y

            @pl.when(f == nf - 1)
            def _():
                x_sc[e, :m, :] = (acc_sc[:m, :] + y).astype(BF)

    s = j - el * nf

    @pl.when(s >= 0)
    def _():
        for e in range(el):
            o = pl.multiple_of(off_ref[s * el + e], 16)
            y_sc[e * cap:(e + 1) * cap, :] = x_sc[e, pl.ds(o, cap), :]
        r, g = r_ref[0], g_ref[0]
        per = 128 // cap
        lane = lax.broadcasted_iota(jnp.int32, (t, 128), 1)
        parts = []
        for q in range(el // per):
            rr, gg = r[:, q * per:q * per + 1], g[:, q * per:q * per + 1]
            for k in range(1, per):
                hit = lane >= k * cap
                rr = jnp.where(hit, r[:, q * per + k:q * per + k + 1], rr)
                gg = jnp.where(hit, g[:, q * per + k:q * per + k + 1], gg)
            parts.append(jnp.where(rr == lane % cap, gg, 0.0))
        gm = jnp.concatenate(parts, axis=1)
        ghi = gm.astype(BF)
        r1 = gm - ghi.astype(F32)
        gmid = r1.astype(BF)
        glo = (r1 - gmid.astype(F32)).astype(BF)
        for c in range(d // 512):
            cs = slice(c * 512, (c + 1) * 512)
            y = y_sc[:, cs]
            o_ref[0, :, cs] = _dot(ghi, y) + (_dot(gmid, y) + _dot(glo, y))


def _experts(u_all, gm, ue1, ue3, ue2, cap):
    ns, t, d = u_all.shape
    el, _, fe = ue1.shape
    mb, nf = 128, 2
    ft = fe // nf
    routed = gm >= 0
    before = (jnp.arange(t)[:, None] > jnp.arange(t)[None, :]).astype(BF)
    rank = jnp.einsum('ab,sbe->sae', before, routed.astype(BF), preferred_element_type=F32).astype(jnp.int32)
    rank = jnp.where(routed, rank, -1)
    cnt = jnp.sum(routed.astype(jnp.int32), axis=1)
    pad = (cnt + 15) // 16 * 16
    off = jnp.cumsum(pad, axis=0) - pad
    nb = jnp.maximum((jnp.sum(pad, axis=0) + mb - 1) // mb, 1)
    steps = ns + el * nf + ns
    wi = lambda i: jnp.clip(i - ns, 0, el * nf - 1)
    gs = pltpu.PrefetchScalarGridSpec(
        num_scalar_prefetch=2,
        grid=(steps,),
        in_specs=[
            pl.BlockSpec((1, t, d), lambda i, *_: (jnp.minimum(i, ns - 1), 0, 0)),
            pl.BlockSpec((1, el, t), lambda i, *_: (jnp.minimum(i, ns - 1), 0, 0)),
            pl.BlockSpec((1, t, el), lambda i, *_: (jnp.maximum(i - ns - el * nf, 0), 0, 0)),
            pl.BlockSpec((1, t, el), lambda i, *_: (jnp.maximum(i - ns - el * nf, 0), 0, 0)),
            pl.BlockSpec((1, d, ft), lambda i, *_: (wi(i) // nf, 0, wi(i) % nf)),
            pl.BlockSpec((1, d, ft), lambda i, *_: (wi(i) // nf, 0, wi(i) % nf)),
            pl.BlockSpec((1, ft, d), lambda i, *_: (wi(i) // nf, wi(i) % nf, 0)),
        ],
        out_specs=pl.BlockSpec((1, t, d), lambda i, *_: (jnp.maximum(i - ns - el * nf, 0), 0, 0)),
        scratch_shapes=[
            pltpu.VMEM((el, ns * cap, d), BF),
            pltpu.VMEM((ns * cap, d), F32),
            pltpu.VMEM((el * cap, d), BF),
        ],
    )
    return pl.pallas_call(
        functools.partial(_expert_kernel, ns=ns, el=el, cap=cap, nf=nf, mb=mb),
        grid_spec=gs,
        out_shape=jax.ShapeDtypeStruct((ns, t, d), F32),
        cost_estimate=pl.CostEstimate(flops=6 * el * ns * cap * d * fe, bytes_accessed=6 * el * d * fe, transcendentals=0),
        compiler_params=pltpu.CompilerParams(dimension_semantics=("arbitrary",), vmem_limit_bytes=60 << 20),
        name="experts",
    )(off.reshape(-1), nb, u_all, rank.transpose(0, 2, 1), rank, gm, ue1, ue3, ue2)


def solution(mesh):
    G = mesh.shape['ep']

    def local(h0, idx, slot, na, wq, wk, wv, wo, nf, w1, w3, w2, nm, wr, ue1, ue3, ue2):
        b, s, d = h0.shape
        t = b * s
        k = idx.shape[-1]
        el = ue1.shape[0]
        ne = el * G
        cap = 2 * t * k // ne
        h = h0.reshape(t, d)
        u = _rms(h, nm)
        logits = _dot(u, wr)
        ix = idx.reshape(t, k)
        hot = ix[:, :, None] == jnp.arange(ne)[None, None, :]
        routed = jnp.any(hot, axis=1)
        lg = jnp.where(routed, logits, -jnp.inf)
        mx = jnp.max(lg, axis=-1, keepdims=True)
        ex = jnp.exp(lg - mx)
        g = ex / jnp.sum(ex, axis=-1, keepdims=True)
        gm = jnp.where(routed, g, -1.0)
        u_all = lax.all_gather(u, 'ep')
        gm_all = lax.all_gather(gm, 'ep')
        me = lax.axis_index('ep')
        gm_loc = lax.dynamic_slice_in_dim(gm_all, me * el, el, axis=2)
        a = _attention(h, na, wq, wk, wv, wo)
        part = _experts(u_all, gm_loc, ue1, ue3, ue2, cap)
        m = lax.psum_scatter(part, 'ep', scatter_dimension=0)
        dense = _ffn(a, nf, w1, w3, w2)
        return (dense + m.reshape(t, d)).astype(BF).reshape(b, s, d)

    rows_spec = P(('dp', 'ep'))
    in_specs = (rows_spec,) * 3 + (P(),) * 11 + (P('ep'),) * 3
    return jax.shard_map(local, mesh=mesh, in_specs=in_specs, out_specs=rows_spec, check_vma=False)
```

```python
import functools

import jax
import jax.numpy as jnp
from jax import lax
from jax.experimental import pallas as pl
from jax.experimental.pallas import tpu as pltpu
from jax.sharding import PartitionSpec as P

HEAD = 128
EPS = 1e-6
ROPE_BASE = 10000.0
F32, BF = jnp.float32, jnp.bfloat16


def _rms(x, w):
    xf = x.astype(F32)
    r = lax.rsqrt(jnp.mean(xf * xf, axis=-1, keepdims=True) + EPS)
    return (xf * r * w.astype(F32)).astype(BF)


def _dot(a, b):
    return jnp.dot(a, b, preferred_element_type=F32)


MESH = pl.DeviceIdType.MESH


def _peer(me, r):
    p = me
    if r & 1:
        p = p + 1 - 2 * (me % 2)
    if r & 2:
        p = p + 2 - 4 * ((me // 2) % 2)
    if r & 4:
        p = p + 4 - 8 * (me // 4)
    return p


def _barrier(me, rels):
    sem = pltpu.get_barrier_semaphore()
    for r in rels:
        pl.semaphore_signal(sem, inc=1, device_id={'ep': _peer(me, r)}, device_id_type=MESH)
    return lambda: pl.semaphore_wait(sem, len(rels))


def _ffn_tile(z, w1, w3, w2):
    h1 = _dot(z, w1)
    h3 = _dot(z, w3)
    hid = (h1 * jax.nn.sigmoid(h1) * h3).astype(BF)
    return _dot(hid, w2)


def _first_kernel(h_ref, na_ref, nm_ref, nf_ref, wr_ref, idx_ref, cos_ref, sin_ref, wq_ref, wk_ref, wv_ref, wo_ref,
                  w1_ref, w3_ref, w2_ref, z_ref, f_ref, uall_ref, gall_ref,
                  x_sc, acc_sc, u_sc, g_sc, sa, ra, sb, rb, sc, rc, sg, rg, ls, *, na_steps, nf_steps, hps, el, step_b, step_c):
    i = pl.program_id(0)
    t, d = h_ref.shape
    me = lax.axis_index('ep')
    hops = (1, 2, 4)
    half = t // 2

    def remote(src, dst, s, r, rel):
        return pltpu.make_async_remote_copy(src_ref=src, dst_ref=dst, send_sem=s, recv_sem=r,
                                            device_id={'ep': _peer(me, rel)}, device_id_type=MESH)

    def stage_a(n):
        return remote(u_sc, uall_ref.at[hops[n]], sa.at[n], ra.at[n], hops[n])

    def stage_g(r):
        rows = pl.ds(pl.multiple_of(_peer(me, r) * el, el), el)
        return remote(g_sc.at[rows], gall_ref.at[r], sg.at[r - 1], rg.at[r - 1], r)

    def stage_b(n):
        rows = pl.ds(n * half, half)
        return remote(uall_ref.at[(2, 4)[n], rows], uall_ref.at[6, rows], sb.at[n], rb.at[n], (4, 2)[n])

    def stage_c(n):
        return remote(uall_ref.at[2 * n + 2], uall_ref.at[2 * n + 3], sc.at[n], rc.at[n], 1)

    def own():
        rows = pl.ds(pl.multiple_of(me * el, el), el)
        return (pltpu.make_async_copy(u_sc, uall_ref.at[0], ls.at[0]),
                pltpu.make_async_copy(g_sc.at[rows], gall_ref.at[0], ls.at[1]))

    @pl.when(i == 0)
    def _():
        arrived = _barrier(me, range(1, 8))
        u = _rms(h_ref[...], nm_ref[...])
        u_sc[...] = u
        logits = _dot(u, wr_ref[...])
        ne = logits.shape[1]
        lane = lax.broadcasted_iota(jnp.int32, (t, ne), 1)
        routed = lane == idx_ref[:, 0:1]
        for j in range(1, idx_ref.shape[1]):
            routed = routed | (lane == idx_ref[:, j:j + 1])
        lg = jnp.where(routed, logits, -jnp.inf)
        ex = jnp.exp(lg - jnp.max(lg, axis=-1, keepdims=True))
        g = jnp.where(routed, ex / jnp.sum(ex, axis=-1, keepdims=True), -1.0)
        g_sc[...] = jnp.transpose(jnp.concatenate([g] * (128 // ne), axis=1))[:ne]
        arrived()
        for n in (1, 2, 0):
            stage_a(n).start()
        for r in range(1, 8):
            stage_g(r).start()
        for c in own():
            c.start()
        x_sc[...] = _rms(h_ref[...], na_ref[...])
        acc_sc[...] = jnp.zeros_like(acc_sc)

    @pl.when(i < na_steps)
    def _():
        x = x_sc[...]
        q2 = _dot(x, wq_ref[...])
        k2 = _dot(x, wk_ref[...])
        v2 = _dot(x, wv_ref[...]).astype(BF)
        cos, sin = cos_ref[...], sin_ref[...]
        causal = lax.broadcasted_iota(jnp.int32, (t, t), 0) >= lax.broadcasted_iota(jnp.int32, (t, t), 1)
        outs = []
        for h in range(hps):
            sl = slice(h * HEAD, (h + 1) * HEAD)
            q, k, v = q2[:, sl], k2[:, sl], v2[:, sl]
            q = (q * cos + pltpu.roll(q, HEAD // 2, 1) * sin).astype(BF)
            k = (k * cos + pltpu.roll(k, HEAD // 2, 1) * sin).astype(BF)
            s = lax.dot_general(q, k, (((1,), (1,)), ((), ())), preferred_element_type=F32) * HEAD ** -0.5
            s = jnp.where(causal, s, -jnp.inf)
            p = jnp.exp(s - jnp.max(s, axis=-1, keepdims=True))
            p = (p / jnp.sum(p, axis=-1, keepdims=True)).astype(BF)
            outs.append(_dot(p, v).astype(BF))
        acc_sc[...] += _dot(jnp.concatenate(outs, axis=1), wo_ref[...])

    @pl.when(i == na_steps - 1)
    def _():
        a = (h_ref[...].astype(F32) + acc_sc[...]).astype(BF)
        f_ref[...] = a.astype(F32)
        z_ref[...] = _rms(a, nf_ref[...])

    @pl.when(i == step_b)
    def _():
        for n in range(2):
            stage_a(n + 1).wait_recv()
            stage_b(n).start()
            stage_c(n).start()

    @pl.when(i == step_c)
    def _():
        for n in range(2):
            stage_b(n).wait_recv()
        stage_c(2).start()

    @pl.when(i >= na_steps)
    def _():
        f_ref[...] += _ffn_tile(z_ref[...], w1_ref[...], w3_ref[...], w2_ref[...])

    @pl.when(i == na_steps + nf_steps - 1)
    def _():
        stage_a(0).wait_recv()
        for n in range(3):
            stage_a(n).wait_send()
        for n in range(2):
            stage_b(n).wait_send()
        for n in range(3):
            stage_c(n).wait()
        for r in range(1, 8):
            stage_g(r).wait()
        for c in own():
            c.wait()


def _first(h, na, nm, nf, wr, idx, wq, wk, wv, wo, w1, w3, w2, el, nf_steps, ft):
    t, d = h.shape
    hps = 2
    w = HEAD * hps
    na_steps = wq.shape[1] // w
    ne = wr.shape[1]
    pos = jnp.arange(t).astype(F32)
    inv = ROPE_BASE ** (-2.0 * jnp.arange(HEAD // 2).astype(F32) / HEAD)
    ang = pos[:, None] * inv[None, :]
    c, s = jnp.cos(ang), jnp.sin(ang)
    cos, sin = jnp.concatenate([c, c], 1), jnp.concatenate([-s, s], 1)
    full = lambda shape: pl.BlockSpec(shape, lambda i: (0, 0))
    ai = lambda i: jnp.minimum(i, na_steps - 1)
    fi = lambda i: jnp.maximum(i - na_steps, 0)
    any_ = pl.BlockSpec(memory_space=pl.ANY)
    dma = pltpu.SemaphoreType.DMA
    return pl.pallas_call(
        functools.partial(_first_kernel, na_steps=na_steps, nf_steps=nf_steps, hps=hps, el=el, step_b=na_steps + 1,
                          step_c=na_steps + nf_steps - 2),
        grid=(na_steps + nf_steps,),
        in_specs=[full((t, d)), full((1, d)), full((1, d)), full((1, d)), full((d, ne)), full(idx.shape),
                  full((t, HEAD)), full((t, HEAD))]
        + [pl.BlockSpec((d, w), lambda i: (0, ai(i)))] * 3
        + [pl.BlockSpec((w, d), lambda i: (ai(i), 0))]
        + [pl.BlockSpec((d, ft), lambda i: (0, fi(i)))] * 2
        + [pl.BlockSpec((ft, d), lambda i: (fi(i), 0))],
        out_specs=[full((t, d)), full((t, d)), any_, any_],
        out_shape=[jax.ShapeDtypeStruct((t, d), BF), jax.ShapeDtypeStruct((t, d), F32),
                   jax.ShapeDtypeStruct((8, t, d), BF), jax.ShapeDtypeStruct((8, el, t), F32)],
        scratch_shapes=[pltpu.VMEM((t, d), BF), pltpu.VMEM((t, d), F32), pltpu.VMEM((t, d), BF),
                        pltpu.VMEM((ne, t), F32),
                        dma((3,)), dma((3,)), dma((2,)), dma((2,)), dma((3,)), dma((3,)), dma((7,)), dma((7,)), dma((2,))],
        cost_estimate=pl.CostEstimate(flops=8 * t * d * d, bytes_accessed=8 * d * d, transcendentals=0),
        compiler_params=pltpu.CompilerParams(dimension_semantics=("arbitrary",), collective_id=0, has_side_effects=True,
                                             vmem_limit_bytes=56 << 20),
        name="first",
    )(h, na.reshape(1, d), nm.reshape(1, d), nf.reshape(1, d), wr, idx, cos, sin, wq, wk, wv, wo, w1, w3, w2)


def _hid_kernel(off_ref, nb_ref, g_ref, u_hbm, w1_hbm, w3_hbm, hid_hbm, gm_hbm,
                u_sc, x_sc, w1_sc, w3_sc, h_sc, hx_sc, gm_sc, su, sw1, sw3, sh, sg, *, ns, el, cap, nf, mb, depth):
    t, d = u_sc.shape[1:]
    ft = w1_sc.shape[-1]
    rows = ns * cap
    total = el * nf

    def fetch(k):
        slot = lax.rem(k, depth)
        e, f = lax.div(k, nf), lax.rem(k, nf)
        cols = pl.ds(pl.multiple_of(f * ft, ft), ft)
        return (pltpu.make_async_copy(w1_hbm.at[e, :, cols], w1_sc.at[slot], sw1.at[slot]),
                pltpu.make_async_copy(w3_hbm.at[e, :, cols], w3_sc.at[slot], sw3.at[slot]))

    def put_h(k):
        slot = lax.rem(k, 2)
        e, f = lax.div(k, nf), lax.rem(k, nf)
        cols = pl.ds(pl.multiple_of(f * ft, ft), ft)
        return pltpu.make_async_copy(hx_sc.at[slot], hid_hbm.at[e, :, cols], sh.at[slot])

    def put_g(s):
        slot = lax.rem(s, 2)
        return pltpu.make_async_copy(gm_sc.at[slot], gm_hbm.at[s], sg.at[slot])

    def get_u(s):
        return pltpu.make_async_copy(u_hbm.at[s], u_sc.at[s], su.at[s])

    for s in range(ns):
        get_u(s).start()
    for k in range(depth):
        for c in fetch(k):
            c.start()
    h_sc[...] = jnp.zeros_like(h_sc)
    it = lax.broadcasted_iota(jnp.int32, (cap, t), 0).astype(F32)
    before = jnp.where(lax.broadcasted_iota(jnp.int32, (t, t), 0) < lax.broadcasted_iota(jnp.int32, (t, t), 1), 1.0, 0.0)

    @pl.loop(0, ns)
    def _(s):
        g = g_ref[s]
        rank = jnp.where(g >= 0, _dot(jnp.where(g >= 0, 1.0, 0.0), before), -1.0)
        hit = [it == rank[e:e + 1, :] for e in range(el)]
        p = jnp.concatenate([jnp.where(h, 1.0, 0.0).astype(BF) for h in hit], axis=0)
        gt = jnp.concatenate([jnp.where(h, g[e:e + 1, :], 0.0) for e, h in enumerate(hit)], axis=0)
        gm = jnp.transpose(gt)
        ghi = gm.astype(BF)
        r1 = gm - ghi.astype(F32)
        gmid = r1.astype(BF)
        glo = (r1 - gmid.astype(F32)).astype(BF)

        @pl.when(s >= 2)
        def _():
            put_g(s - 2).wait()
        gm_sc[lax.rem(s, 2)] = jnp.concatenate([ghi, gmid, glo], axis=1)
        put_g(s).start()
        get_u(s).wait()
        for c in range(d // 512):
            cs = slice(c * 512, (c + 1) * 512)
            xv = _dot(p, u_sc[s, :, cs]).astype(BF)
            for e in range(el):
                o = pl.multiple_of(off_ref[s * el + e], 16)
                x_sc[e, pl.ds(o, cap), cs] = xv[e * cap:(e + 1) * cap]

    @pl.loop(0, total)
    def _(k):
        slot = lax.rem(k, depth)
        e = lax.div(k, nf)
        for c in fetch(k):
            c.wait()
        for m in range(mb, rows + 1, mb):
            @pl.when(nb_ref[e] == m // mb)
            def _():
                x = x_sc[e, :m, :]
                h1 = _dot(x, w1_sc[slot])
                h3 = _dot(x, w3_sc[slot])
                h_sc[:m, :] = (h1 * jax.nn.sigmoid(h1) * h3).astype(BF)

        @pl.when(k + depth < total)
        def _():
            for c in fetch(k + depth):
                c.start()

        @pl.when(k >= 2)
        def _():
            put_h(k - 2).wait()
        for s in range(ns):
            o = pl.multiple_of(off_ref[s * el + e], 16)
            hx_sc[lax.rem(k, 2), s * cap:(s + 1) * cap, :] = h_sc[pl.ds(o, cap), :]
        put_h(k).start()

    for s in (ns - 2, ns - 1):
        put_g(s).wait()
    for k in (total - 2, total - 1):
        put_h(k).wait()


def _hidden(u_all, g_all, ue1, ue3, cap):
    ns, t, d = u_all.shape
    el, _, fe = ue1.shape
    mb, nf, depth = 128, 2, 4
    ft = fe // nf
    cnt = jnp.sum((g_all >= 0).astype(jnp.int32), axis=-1)
    pad = (cnt + 15) // 16 * 16
    off = jnp.cumsum(pad, axis=0) - pad
    nb = jnp.maximum((jnp.sum(pad, axis=0) + mb - 1) // mb, 1)
    smem, vmem, any_ = (pl.BlockSpec(memory_space=m) for m in (pltpu.SMEM, pltpu.VMEM, pl.ANY))
    dma = pltpu.SemaphoreType.DMA
    return pl.pallas_call(
        functools.partial(_hid_kernel, ns=ns, el=el, cap=cap, nf=nf, mb=mb, depth=depth),
        in_specs=[smem, smem, vmem, any_, any_, any_],
        out_specs=[any_, any_],
        out_shape=[jax.ShapeDtypeStruct((el, ns * cap, fe), BF), jax.ShapeDtypeStruct((ns, t, 3 * el * cap), BF)],
        scratch_shapes=[pltpu.VMEM((ns, t, d), BF), pltpu.VMEM((el, ns * cap, d), BF), pltpu.VMEM((depth, d, ft), BF),
                        pltpu.VMEM((depth, d, ft), BF), pltpu.VMEM((ns * cap, ft), BF), pltpu.VMEM((2, ns * cap, ft), BF),
                        pltpu.VMEM((2, t, 3 * el * cap), BF),
                        dma((ns,)), dma((depth,)), dma((depth,)), dma((2,)), dma((2,))],
        cost_estimate=pl.CostEstimate(flops=4 * el * ns * cap * d * fe, bytes_accessed=4 * el * d * fe, transcendentals=0),
        compiler_params=pltpu.CompilerParams(vmem_limit_bytes=58 << 20),
        name="hidden",
    )(off.reshape(-1), nb, g_all, u_all, ue1, ue3)


E0 = {q: q + 1 for q in range(8)}
E1 = {0: 4, 1: 4, 2: 5, 3: 6, 4: 7, 5: 11, 6: 12, 7: 12}
E2 = {0: 8, 1: 8, 2: 9, 3: 10, 4: 12, 5: 12, 6: 12, 7: 12}
NQ, F_FROM, STEPS = 8, 4, 13


def _last_kernel(hid_hbm, gm_hbm, z_ref, f_ref, ue2_ref, w1_ref, w3_ref, w2_ref, o_ref,
                 hid_sc, gm_sc, y_sc, keep_sc, ps_sc, r0_sc, r1_sc, r2_sc, acc_sc, hs, gs, s0, r0, s1, r1, s2, r2,
                 *, ns, el, cap, nfs):
    i = pl.program_id(0)
    t, d = z_ref.shape
    cw = ue2_ref.shape[-1]
    me = lax.axis_index('ep')

    def get_h(e):
        return pltpu.make_async_copy(hid_hbm.at[e], hid_sc.at[e], hs.at[e])

    def get_g(s):
        return pltpu.make_async_copy(gm_hbm.at[s], gm_sc.at[s], gs.at[s])

    def remote(src, dst, s, r, dev):
        return pltpu.make_async_remote_copy(src_ref=src, dst_ref=dst, send_sem=s, recv_sem=r,
                                            device_id={'ep': dev}, device_id_type=MESH)

    def turn(q, even, odd):
        return even if q % 2 == 0 else odd

    def send0(q, slot):
        return remote(ps_sc.at[slot], r0_sc.at[q], s0.at[q], r0.at[q], _peer(me, 1))

    def send1(q):
        return remote(r0_sc.at[q, pl.ds(2, 2)], r1_sc.at[q], s1.at[q], r1.at[q], _peer(me, turn(q, 2, 4)))

    def send2(q):
        return remote(r0_sc.at[q, 1], r2_sc.at[q], s2.at[q], r2.at[q], _peer(me, turn(q, 4, 2)))

    @pl.when(i == 0)
    def _():
        arrived = _barrier(me, (1, 2, 4))
        for e in range(el):
            get_h(e).start()
        for s in range(ns):
            get_g(s).start()
        acc_sc[...] = f_ref[...]
        arrived()

    @pl.when(i < NQ)
    def _():
        for e in range(el):
            @pl.when(i == 0)
            def _():
                get_h(e).wait()
            y = _dot(hid_sc[e], ue2_ref[e]).astype(BF)
            for s in range(ns):
                y_sc[s, e * cap:(e + 1) * cap, :] = y[s * cap:(s + 1) * cap]

    for q, step in E0.items():
        @pl.when(i == step)
        def _():
            send0(q, q % 2).wait_recv()
            r0_sc[q] += keep_sc[...]
            send1(q).start()

    @pl.when(i == 0)
    def _():
        for s in range(ns):
            get_g(s).wait()

    @pl.when((i >= 2) & (i < NQ))
    def _():
        send0(i - 2, i % 2).wait_send()

    @pl.when(i < NQ)
    def _():
        odd = i % 2
        kk = el * cap
        for b in range(4):
            for c in range(2):
                s = c + (0, 4 - 2 * odd, 2 + 2 * odd, 6)[b]
                y = y_sc[s]
                m = _dot(gm_sc[s, :, :kk], y) + _dot(gm_sc[s, :, kk:2 * kk], y) + _dot(gm_sc[s, :, 2 * kk:], y)
                if c == 0:
                    keep_sc[b] = m
                else:
                    ps_sc[i % 2, b] = m
        send0(i, i % 2).start()

    @pl.when((i >= F_FROM) & (i < F_FROM + nfs))
    def _():
        acc_sc[...] += _ffn_tile(z_ref[...], w1_ref[...], w3_ref[...], w2_ref[...])

    for q, step in E1.items():
        @pl.when(i == step)
        def _():
            send1(q).wait_recv()
            r0_sc[q, 0:2] += r1_sc[q]
            send2(q).start()

    for q, step in E2.items():
        @pl.when(i == step)
        def _():
            send2(q).wait_recv()
            acc_sc[:, q * cw:(q + 1) * cw] += r0_sc[q, 0] + r2_sc[q]

    @pl.when(i == STEPS - 1)
    def _():
        for q in (NQ - 2, NQ - 1):
            send0(q, q % 2).wait_send()
        for q in range(NQ):
            send1(q).wait_send()
            send2(q).wait_send()
        o_ref[...] = acc_sc[...].astype(BF)


def _last(hid, gm, z, f, ue2, w1, w3, w2, cap, ft, f0):
    t, d = z.shape
    el, rows, fe = hid.shape
    ns = rows // cap
    cw = d // NQ
    nfs = w1.shape[1] // ft - f0
    full = lambda shape: pl.BlockSpec(shape, lambda i: (0, 0), pipeline_mode=pl.Buffered(1))
    qi = lambda i: jnp.minimum(i, NQ - 1)
    fi = lambda i: f0 + jnp.clip(i - F_FROM, 0, nfs - 1)
    any_ = pl.BlockSpec(memory_space=pl.ANY)
    dma = pltpu.SemaphoreType.DMA
    return pl.pallas_call(
        functools.partial(_last_kernel, ns=ns, el=el, cap=cap, nfs=nfs),
        grid=(STEPS,),
        in_specs=[any_, any_, full((t, d)), full((t, d)),
                  pl.BlockSpec((el, fe, cw), lambda i: (0, 0, qi(i)))]
        + [pl.BlockSpec((d, ft), lambda i: (0, fi(i)))] * 2
        + [pl.BlockSpec((ft, d), lambda i: (fi(i), 0))],
        out_specs=full((t, d)),
        out_shape=jax.ShapeDtypeStruct((t, d), BF),
        scratch_shapes=[pltpu.VMEM((el, rows, fe), BF), pltpu.VMEM(gm.shape, BF), pltpu.VMEM((ns, el * cap, cw), BF),
                        pltpu.VMEM((4, t, cw), F32), pltpu.VMEM((2, 4, t, cw), F32), pltpu.VMEM((NQ, 4, t, cw), F32),
                        pltpu.VMEM((NQ, 2, t, cw), F32), pltpu.VMEM((NQ, t, cw), F32), pltpu.VMEM((t, d), F32),
                        dma((el,)), dma((ns,))] + [dma((NQ,))] * 6,
        cost_estimate=pl.CostEstimate(flops=2 * el * rows * d * fe, bytes_accessed=2 * el * d * fe, transcendentals=0),
        compiler_params=pltpu.CompilerParams(dimension_semantics=("arbitrary",), collective_id=1, has_side_effects=True,
                                             vmem_limit_bytes=67043328),
        name="last",
    )(hid, gm, z, f, ue2, w1, w3, w2)


def solution(mesh):
    G = mesh.shape['ep']
    ft, f0 = 512, 8

    def local(h0, idx, slot, na, wq, wk, wv, wo, nf, w1, w3, w2, nm, wr, ue1, ue3, ue2):
        b, s, d = h0.shape
        t = b * s
        k = idx.shape[-1]
        el = ue1.shape[0]
        cap = 2 * t * k // (el * G)
        z, f, u_all, g_all = _first(h0.reshape(t, d), na, nm, nf, wr, idx.reshape(t, k), wq, wk, wv, wo, w1, w3, w2,
                                    el, f0, ft)
        hid, gm = _hidden(u_all, g_all, ue1, ue3, cap)
        return _last(hid, gm, z, f, ue2, w1, w3, w2, cap, ft, f0).reshape(b, s, d)

    rows_spec = P(('dp', 'ep'))
    in_specs = (rows_spec,) * 3 + (P(),) * 11 + (P('ep'),) * 3
    return jax.shard_map(local, mesh=mesh, in_specs=in_specs, out_specs=rows_spec, check_vma=False)
```

```python
import functools

import jax
import jax.numpy as jnp
from jax import lax
from jax.experimental import pallas as pl
from jax.experimental.pallas import tpu as pltpu
from jax.sharding import PartitionSpec as P

HEAD = 128
EPS = 1e-6
ROPE_BASE = 10000.0
F32, BF = jnp.float32, jnp.bfloat16


def _rms(x, w):
    xf = x.astype(F32)
    r = lax.rsqrt(jnp.mean(xf * xf, axis=-1, keepdims=True) + EPS)
    return (xf * r * w.astype(F32).reshape(1, -1)).astype(BF)


def _dot(a, b):
    return jnp.dot(a, b, preferred_element_type=F32)


MESH = pl.DeviceIdType.MESH


def _peer(me, r):
    p = me
    if r & 1:
        p = p + 1 - 2 * (me % 2)
    if r & 2:
        p = p + 2 - 4 * ((me // 2) % 2)
    if r & 4:
        p = p + 4 - 8 * (me // 4)
    return p


def _barrier(me, rels):
    sem = pltpu.get_barrier_semaphore()
    for r in rels:
        pl.semaphore_signal(sem, inc=1, device_id={'ep': _peer(me, r)}, device_id_type=MESH)
    return lambda: pl.semaphore_wait(sem, len(rels))


class _Tiles:
    def __init__(self, hbm, vmem, sems, first, count):
        self.hbm, self.vmem, self.sems, self.first, self.count = hbm, vmem, sems, first, count

    def copies(self, k):
        slot = lax.rem(k, 2)
        ft = self.vmem[0].shape[-1]
        part = pl.ds(pl.multiple_of((self.first + k) * ft, ft), ft)
        w1, w3, w2 = self.hbm
        src = (w1.at[:, part], w3.at[:, part], w2.at[part])
        return [pltpu.make_async_copy(a, b.at[slot], c.at[slot]) for a, b, c in zip(src, self.vmem, self.sems)]

    def start(self, k):
        for c in self.copies(k):
            c.start()

    def add(self, k, z, acc_ref):
        for c in self.copies(k):
            c.wait()
        slot = lax.rem(k, 2)
        acc_ref[...] += _ffn_tile(z, *(v[slot] for v in self.vmem))

        @pl.when(k + 2 < self.count)
        def _():
            self.start(k + 2)


def _tile_scratch(d, ft):
    dma = pltpu.SemaphoreType.DMA
    return [pltpu.VMEM((2, d, ft), BF), pltpu.VMEM((2, d, ft), BF), pltpu.VMEM((2, ft, d), BF), dma((2,)), dma((2,)), dma((2,))]


def _ffn_tile(z, w1, w3, w2):
    h1 = _dot(z, w1)
    h3 = _dot(z, w3)
    hid = (h1 * jax.nn.sigmoid(h1) * h3).astype(BF)
    return _dot(hid, w2)


def _first_kernel(h_ref, na_ref, nm_ref, nf_ref, wr_ref, idx_ref, cos_ref, sin_ref, wq_ref, wk_ref, wv_ref, wo_ref,
                  w1_hbm, w3_hbm, w2_hbm, z_ref, f_ref, uall_ref, gall_ref,
                  x_sc, acc_sc, u_sc, g_sc, sa, ra, sb, rb, sc, rc, sg, rg, ls, t1, t3, t2, q1, q3, q2s,
                  *, na_steps, nf_steps, hps, el, step_b, step_c):
    i = pl.program_id(0)
    t, d = h_ref.shape
    me = lax.axis_index('ep')
    hops = (1, 2, 4)
    half = t // 2
    tiles = _Tiles((w1_hbm, w3_hbm, w2_hbm), (t1, t3, t2), (q1, q3, q2s), 0, nf_steps)

    def remote(src, dst, s, r, rel):
        return pltpu.make_async_remote_copy(src_ref=src, dst_ref=dst, send_sem=s, recv_sem=r,
                                            device_id={'ep': _peer(me, rel)}, device_id_type=MESH)

    def stage_a(n):
        return remote(u_sc, uall_ref.at[hops[n]], sa.at[n], ra.at[n], hops[n])

    def stage_g(r):
        rows = pl.ds(pl.multiple_of(_peer(me, r) * el, el), el)
        return remote(g_sc.at[rows], gall_ref.at[r], sg.at[r - 1], rg.at[r - 1], r)

    def stage_b(n):
        rows = pl.ds(n * half, half)
        return remote(uall_ref.at[(2, 4)[n], rows], uall_ref.at[6, rows], sb.at[n], rb.at[n], (4, 2)[n])

    def stage_c(n):
        return remote(uall_ref.at[2 * n + 2], uall_ref.at[2 * n + 3], sc.at[n], rc.at[n], 1)

    def own():
        rows = pl.ds(pl.multiple_of(me * el, el), el)
        return (pltpu.make_async_copy(u_sc, uall_ref.at[0], ls.at[0]),
                pltpu.make_async_copy(g_sc.at[rows], gall_ref.at[0], ls.at[1]))

    @pl.when(i == 0)
    def _():
        arrived = _barrier(me, range(1, 8))
        u = _rms(h_ref[...], nm_ref[...])
        u_sc[...] = u
        logits = lax.dot_general(wr_ref[...], u, (((1,), (1,)), ((), ())), preferred_element_type=F32)
        row = lax.broadcasted_iota(jnp.int32, logits.shape, 0)
        routed = row == idx_ref[0:1, :]
        for j in range(1, idx_ref.shape[0]):
            routed = routed | (row == idx_ref[j:j + 1, :])
        lg = jnp.where(routed, logits, -jnp.inf)
        ex = jnp.exp(lg - jnp.max(lg, axis=0, keepdims=True))
        g_sc[...] = jnp.where(routed, ex / jnp.sum(ex, axis=0, keepdims=True), -1.0)
        arrived()
        for n in (1, 2, 0):
            stage_a(n).start()
        for r in range(1, 8):
            stage_g(r).start()
        for c in own():
            c.start()
        x_sc[...] = _rms(h_ref[...], na_ref[...])
        acc_sc[...] = jnp.zeros_like(acc_sc)

    @pl.when(i < na_steps)
    def _():
        x = x_sc[...]
        q2 = _dot(x, wq_ref[...])
        k2 = _dot(x, wk_ref[...])
        v2 = _dot(x, wv_ref[...]).astype(BF)
        cos, sin = cos_ref[...], sin_ref[...]
        causal = lax.broadcasted_iota(jnp.int32, (t, t), 0) >= lax.broadcasted_iota(jnp.int32, (t, t), 1)
        outs = []
        for h in range(hps):
            sl = slice(h * HEAD, (h + 1) * HEAD)
            q, k, v = q2[:, sl], k2[:, sl], v2[:, sl]
            q = (q * cos + pltpu.roll(q, HEAD // 2, 1) * sin).astype(BF)
            k = (k * cos + pltpu.roll(k, HEAD // 2, 1) * sin).astype(BF)
            s = lax.dot_general(q, k, (((1,), (1,)), ((), ())), preferred_element_type=F32) * HEAD ** -0.5
            s = jnp.where(causal, s, -jnp.inf)
            p = jnp.exp(s - jnp.max(s, axis=-1, keepdims=True))
            p = (p / jnp.sum(p, axis=-1, keepdims=True)).astype(BF)
            outs.append(_dot(p, v).astype(BF))
        acc_sc[...] += _dot(jnp.concatenate(outs, axis=1), wo_ref[...])

    @pl.when(i == na_steps - 1)
    def _():
        a = (h_ref[...].astype(F32) + acc_sc[...]).astype(BF)
        f_ref[...] = a.astype(F32)
        z_ref[...] = _rms(a, nf_ref[...])

    @pl.when(i == step_b)
    def _():
        for n in range(2):
            stage_a(n + 1).wait_recv()
            stage_b(n).start()
            stage_c(n).start()

    @pl.when(i == step_c)
    def _():
        for n in range(2):
            stage_b(n).wait_recv()
        stage_c(2).start()

    @pl.when(i == na_steps - 3)
    def _():
        tiles.start(0)
        tiles.start(1)

    @pl.when((i >= na_steps) & (i < na_steps + nf_steps))
    def _():
        tiles.add(i - na_steps, z_ref[...], f_ref)

    @pl.when(i == na_steps + nf_steps)
    def _():
        stage_a(0).wait_recv()
        for n in range(3):
            stage_a(n).wait_send()
        for n in range(2):
            stage_b(n).wait_send()
        for n in range(3):
            stage_c(n).wait()
        for r in range(1, 8):
            stage_g(r).wait()
        for c in own():
            c.wait()


def _first(h, na, nm, nf, wr, idx, wq, wk, wv, wo, w1, w3, w2, el, nf_steps, ft):
    t, d = h.shape
    hps = 2
    w = HEAD * hps
    na_steps = wq.shape[1] // w
    ne = wr.shape[0]
    pos = jnp.arange(t).astype(F32)
    inv = ROPE_BASE ** (-2.0 * jnp.arange(HEAD // 2).astype(F32) / HEAD)
    ang = pos[:, None] * inv[None, :]
    c, s = jnp.cos(ang), jnp.sin(ang)
    cos, sin = jnp.concatenate([c, c], 1), jnp.concatenate([-s, s], 1)
    full = lambda shape: pl.BlockSpec(shape, lambda i: (0, 0))
    vec = pl.BlockSpec((d,), lambda i: (0,))
    ai = lambda i: jnp.minimum(i, na_steps - 1)
    any_ = pl.BlockSpec(memory_space=pl.ANY)
    dma = pltpu.SemaphoreType.DMA
    return pl.pallas_call(
        functools.partial(_first_kernel, na_steps=na_steps, nf_steps=nf_steps, hps=hps, el=el, step_b=na_steps,
                          step_c=na_steps + nf_steps),
        grid=(na_steps + nf_steps + 1,),
        in_specs=[full((t, d)), vec, vec, vec, full((ne, d)), full(idx.shape),
                  full((t, HEAD)), full((t, HEAD))]
        + [pl.BlockSpec((d, w), lambda i: (0, ai(i)))] * 3
        + [pl.BlockSpec((w, d), lambda i: (ai(i), 0))]
        + [any_] * 3,
        out_specs=[full((t, d)), full((t, d)), any_, any_],
        out_shape=[jax.ShapeDtypeStruct((t, d), BF), jax.ShapeDtypeStruct((t, d), F32),
                   jax.ShapeDtypeStruct((8, t, d), BF), jax.ShapeDtypeStruct((8, el, t), F32)],
        scratch_shapes=[pltpu.VMEM((t, d), BF), pltpu.VMEM((t, d), F32), pltpu.VMEM((t, d), BF),
                        pltpu.VMEM((ne, t), F32),
                        dma((3,)), dma((3,)), dma((2,)), dma((2,)), dma((3,)), dma((3,)), dma((7,)), dma((7,)), dma((2,))] + _tile_scratch(d, ft),
        cost_estimate=pl.CostEstimate(flops=8 * t * d * d, bytes_accessed=8 * d * d, transcendentals=0),
        compiler_params=pltpu.CompilerParams(dimension_semantics=("arbitrary",), collective_id=0, has_side_effects=True,
                                             vmem_limit_bytes=56 << 20),
        name="first",
    )(h, na, nm, nf, wr, idx, cos, sin, wq, wk, wv, wo, w1, w3, w2)


def _hid_kernel(off_ref, nb_ref, g_ref, u_hbm, w1_hbm, w3_hbm, hid_hbm, gm_hbm,
                u_sc, x_sc, w1_sc, w3_sc, h_sc, hx_sc, gm_sc, su, sw1, sw3, sh, sg, *, ns, el, cap, nf, mb, depth):
    t, d = u_sc.shape[1:]
    ft = w1_sc.shape[-1]
    rows = ns * cap
    total = el * nf

    def fetch(k):
        slot = lax.rem(k, depth)
        e, f = lax.div(k, nf), lax.rem(k, nf)
        cols = pl.ds(pl.multiple_of(f * ft, ft), ft)
        return (pltpu.make_async_copy(w1_hbm.at[e, :, cols], w1_sc.at[slot], sw1.at[slot]),
                pltpu.make_async_copy(w3_hbm.at[e, :, cols], w3_sc.at[slot], sw3.at[slot]))

    def put_h(k):
        slot = lax.rem(k, 2)
        e, f = lax.div(k, nf), lax.rem(k, nf)
        cols = pl.ds(pl.multiple_of(f * ft, ft), ft)
        return pltpu.make_async_copy(hx_sc.at[slot], hid_hbm.at[e, :, cols], sh.at[slot])

    def put_g(s):
        slot = lax.rem(s, 2)
        return pltpu.make_async_copy(gm_sc.at[slot], gm_hbm.at[s], sg.at[slot])

    def get_u(s):
        return pltpu.make_async_copy(u_hbm.at[s], u_sc.at[s], su.at[s])

    for s in range(ns):
        get_u(s).start()
    for k in range(depth):
        for c in fetch(k):
            c.start()
    h_sc[...] = jnp.zeros_like(h_sc)
    it = lax.broadcasted_iota(jnp.int32, (cap, t), 0).astype(F32)
    before = jnp.where(lax.broadcasted_iota(jnp.int32, (t, t), 0) < lax.broadcasted_iota(jnp.int32, (t, t), 1), 1.0, 0.0)

    @pl.loop(0, ns)
    def _(s):
        g = g_ref[s]
        rank = jnp.where(g >= 0, _dot(jnp.where(g >= 0, 1.0, 0.0), before), -1.0)
        hit = [it == rank[e:e + 1, :] for e in range(el)]
        p = jnp.concatenate([jnp.where(h, 1.0, 0.0).astype(BF) for h in hit], axis=0)
        gt = jnp.concatenate([jnp.where(h, g[e:e + 1, :], 0.0) for e, h in enumerate(hit)], axis=0)
        gm = jnp.transpose(gt)
        ghi = gm.astype(BF)
        r1 = gm - ghi.astype(F32)
        gmid = r1.astype(BF)
        glo = (r1 - gmid.astype(F32)).astype(BF)

        @pl.when(s >= 2)
        def _():
            put_g(s - 2).wait()
        gm_sc[lax.rem(s, 2)] = jnp.concatenate([ghi, gmid, glo], axis=1)
        put_g(s).start()
        get_u(s).wait()
        for c in range(d // 512):
            cs = slice(c * 512, (c + 1) * 512)
            xv = _dot(p, u_sc[s, :, cs]).astype(BF)
            for e in range(el):
                o = pl.multiple_of(off_ref[s * el + e], 16)
                x_sc[e, pl.ds(o, cap), cs] = xv[e * cap:(e + 1) * cap]

    @pl.loop(0, total)
    def _(k):
        slot = lax.rem(k, depth)
        e = lax.div(k, nf)
        for c in fetch(k):
            c.wait()
        for m in range(mb, rows + 1, mb):
            @pl.when(nb_ref[e] == m // mb)
            def _():
                x = x_sc[e, :m, :]
                h1 = _dot(x, w1_sc[slot])
                h3 = _dot(x, w3_sc[slot])
                h_sc[:m, :] = (h1 * jax.nn.sigmoid(h1) * h3).astype(BF)

        @pl.when(k + depth < total)
        def _():
            for c in fetch(k + depth):
                c.start()

        @pl.when(k >= 2)
        def _():
            put_h(k - 2).wait()
        for s in range(ns):
            o = pl.multiple_of(off_ref[s * el + e], 16)
            hx_sc[lax.rem(k, 2), s * cap:(s + 1) * cap, :] = h_sc[pl.ds(o, cap), :]
        put_h(k).start()

    for s in (ns - 2, ns - 1):
        put_g(s).wait()
    for k in (total - 2, total - 1):
        put_h(k).wait()


def _hidden(u_all, g_all, ue1, ue3, cap):
    ns, t, d = u_all.shape
    el, _, fe = ue1.shape
    mb, nf, depth = 128, 2, 4
    ft = fe // nf
    cnt = jnp.sum((g_all >= 0).astype(jnp.int32), axis=-1)
    pad = (cnt + 15) // 16 * 16
    off = jnp.cumsum(pad, axis=0) - pad
    nb = jnp.maximum((jnp.sum(pad, axis=0) + mb - 1) // mb, 1)
    smem, vmem, any_ = (pl.BlockSpec(memory_space=m) for m in (pltpu.SMEM, pltpu.VMEM, pl.ANY))
    dma = pltpu.SemaphoreType.DMA
    return pl.pallas_call(
        functools.partial(_hid_kernel, ns=ns, el=el, cap=cap, nf=nf, mb=mb, depth=depth),
        in_specs=[smem, smem, vmem, any_, any_, any_],
        out_specs=[any_, any_],
        out_shape=[jax.ShapeDtypeStruct((el, ns * cap, fe), BF), jax.ShapeDtypeStruct((ns, t, 3 * el * cap), BF)],
        scratch_shapes=[pltpu.VMEM((ns, t, d), BF), pltpu.VMEM((el, ns * cap, d), BF), pltpu.VMEM((depth, d, ft), BF),
                        pltpu.VMEM((depth, d, ft), BF), pltpu.VMEM((ns * cap, ft), BF), pltpu.VMEM((2, ns * cap, ft), BF),
                        pltpu.VMEM((2, t, 3 * el * cap), BF),
                        dma((ns,)), dma((depth,)), dma((depth,)), dma((2,)), dma((2,))],
        cost_estimate=pl.CostEstimate(flops=4 * el * ns * cap * d * fe, bytes_accessed=4 * el * d * fe, transcendentals=0),
        compiler_params=pltpu.CompilerParams(vmem_limit_bytes=58 << 20),
        name="hidden",
    )(off.reshape(-1), nb, g_all, u_all, ue1, ue3)


E0 = {q: q + 1 for q in range(8)}
E1 = {0: 4, 1: 4, 2: 5, 3: 6, 4: 8, 5: 10, 6: 14, 7: 16}
E2 = {0: 8, 1: 8, 2: 12, 3: 12, 4: 15, 5: 16, 6: 16, 7: 16}
NQ, F_FROM, STEPS = 8, 4, 17


def _last_kernel(hid_hbm, gm_hbm, z_ref, f_ref, ue2_ref, w1_hbm, w3_hbm, w2_hbm, o_ref,
                 hid_sc, gm_sc, y_sc, keep_sc, ps_sc, r0_sc, r1_sc, r2_sc, acc_sc, hs, gs, s0, r0, s1, r1, s2, r2,
                 t1, t3, t2, q1, q3, q2s, *, ns, el, cap, f0, nfs):
    i = pl.program_id(0)
    t, d = z_ref.shape
    cw = ue2_ref.shape[-1]
    me = lax.axis_index('ep')
    tiles = _Tiles((w1_hbm, w3_hbm, w2_hbm), (t1, t3, t2), (q1, q3, q2s), f0, nfs)

    def get_h(e):
        return pltpu.make_async_copy(hid_hbm.at[e], hid_sc.at[e], hs.at[e])

    def get_g(s):
        return pltpu.make_async_copy(gm_hbm.at[s], gm_sc.at[s], gs.at[s])

    def remote(src, dst, s, r, dev):
        return pltpu.make_async_remote_copy(src_ref=src, dst_ref=dst, send_sem=s, recv_sem=r,
                                            device_id={'ep': dev}, device_id_type=MESH)

    def turn(q, even, odd):
        return even if q % 2 == 0 else odd

    def send0(q, slot):
        return remote(ps_sc.at[slot], r0_sc.at[q], s0.at[q], r0.at[q], _peer(me, 1))

    def send1(q):
        return remote(r0_sc.at[q, pl.ds(2, 2)], r1_sc.at[q], s1.at[q], r1.at[q], _peer(me, turn(q, 2, 4)))

    def send2(q):
        return remote(r0_sc.at[q, 1], r2_sc.at[q], s2.at[q], r2.at[q], _peer(me, turn(q, 4, 2)))

    @pl.when(i == 0)
    def _():
        arrived = _barrier(me, (1, 2, 4))
        for e in range(el):
            get_h(e).start()
        for s in range(ns):
            get_g(s).start()
        acc_sc[...] = f_ref[...]
        arrived()
        for e in range(el):
            get_h(e).wait()

    def pass_on(qs):
        for q in qs:
            @pl.when(i == E0[q])
            def _():
                send0(q, q % 2).wait_recv()
                r0_sc[q] += keep_sc[...]
                send1(q).start()

    pass_on((0, 1))

    @pl.when(i < NQ)
    def _():
        for e in range(el):
            y = _dot(hid_sc[e], ue2_ref[e]).astype(BF)
            for s in range(ns):
                y_sc[s, e * cap:(e + 1) * cap, :] = y[s * cap:(s + 1) * cap]

    pass_on(range(2, NQ))

    @pl.when(i == 0)
    def _():
        for s in range(ns):
            get_g(s).wait()
        tiles.start(0)
        tiles.start(1)

    @pl.when((i >= 2) & (i < NQ))
    def _():
        send0(i - 2, i % 2).wait_send()

    @pl.when(i < NQ)
    def _():
        odd = i % 2
        kk = el * cap
        for b in range(4):
            for c in range(2):
                s = c + (0, 4 - 2 * odd, 2 + 2 * odd, 6)[b]
                y = y_sc[s]
                m = _dot(gm_sc[s, :, :kk], y) + _dot(gm_sc[s, :, kk:2 * kk], y) + _dot(gm_sc[s, :, 2 * kk:], y)
                if c == 0:
                    keep_sc[b] = m
                else:
                    ps_sc[i % 2, b] = m
        send0(i, i % 2).start()

    @pl.when((i >= F_FROM) & (i < F_FROM + nfs))
    def _():
        tiles.add(i - F_FROM, z_ref[...], acc_sc)

    for q, step in E1.items():
        @pl.when(i == step)
        def _():
            send1(q).wait_recv()
            r0_sc[q, 0:2] += r1_sc[q]
            send2(q).start()

    for q, step in E2.items():
        @pl.when(i == step)
        def _():
            send2(q).wait_recv()
            acc_sc[:, q * cw:(q + 1) * cw] += r0_sc[q, 0] + r2_sc[q]

    @pl.when(i == STEPS - 1)
    def _():
        for q in (NQ - 2, NQ - 1):
            send0(q, q % 2).wait_send()
        for q in range(NQ):
            send1(q).wait_send()
            send2(q).wait_send()
        o_ref[...] = acc_sc[...].astype(BF)


def _last(hid, gm, z, f, ue2, w1, w3, w2, cap, ft, f0):
    t, d = z.shape
    el, rows, fe = hid.shape
    ns = rows // cap
    cw = d // NQ
    nfs = w1.shape[1] // ft - f0
    full = lambda shape: pl.BlockSpec(shape, lambda i: (0, 0), pipeline_mode=pl.Buffered(1))
    qi = lambda i: jnp.minimum(i, NQ - 1)
    any_ = pl.BlockSpec(memory_space=pl.ANY)
    dma = pltpu.SemaphoreType.DMA
    return pl.pallas_call(
        functools.partial(_last_kernel, ns=ns, el=el, cap=cap, f0=f0, nfs=nfs),
        grid=(STEPS,),
        in_specs=[any_, any_, full((t, d)), full((t, d)),
                  pl.BlockSpec((el, fe, cw), lambda i: (0, 0, qi(i)))] + [any_] * 3,
        out_specs=full((t, d)),
        out_shape=jax.ShapeDtypeStruct((t, d), BF),
        scratch_shapes=[pltpu.VMEM((el, rows, fe), BF), pltpu.VMEM(gm.shape, BF), pltpu.VMEM((ns, el * cap, cw), BF),
                        pltpu.VMEM((4, t, cw), F32), pltpu.VMEM((2, 4, t, cw), F32), pltpu.VMEM((NQ, 4, t, cw), F32),
                        pltpu.VMEM((NQ, 2, t, cw), F32), pltpu.VMEM((NQ, t, cw), F32), pltpu.VMEM((t, d), F32),
                        dma((el,)), dma((ns,))] + [dma((NQ,))] * 6 + _tile_scratch(d, ft),
        cost_estimate=pl.CostEstimate(flops=2 * el * rows * d * fe, bytes_accessed=2 * el * d * fe, transcendentals=0),
        compiler_params=pltpu.CompilerParams(dimension_semantics=("arbitrary",), collective_id=1, has_side_effects=True,
                                             vmem_limit_bytes=67043328),
        name="last",
    )(hid, gm, z, f, ue2, w1, w3, w2)


def solution(mesh):
    G = mesh.shape['ep']
    ft, f0 = 512, 4

    def local(h0, idx, slot, na, wq, wk, wv, wo, nf, w1, w3, w2, nm, wr, ue1, ue3, ue2):
        b, s, d = h0.shape
        t = b * s
        k = idx.shape[-1]
        el = ue1.shape[0]
        cap = 2 * t * k // (el * G)
        z, f, u_all, g_all = _first(h0.reshape(t, d), na, nm, nf, wr.T, idx.reshape(t, k).T, wq, wk, wv, wo, w1, w3, w2,
                                    el, f0, ft)
        hid, gm = _hidden(u_all, g_all, ue1, ue3, cap)
        return _last(hid, gm, z, f, ue2, w1, w3, w2, cap, ft, f0).reshape(b, s, d)

    rows_spec = P(('dp', 'ep'))
    in_specs = (rows_spec,) * 3 + (P(),) * 11 + (P('ep'),) * 3
    return jax.shard_map(local, mesh=mesh, in_specs=in_specs, out_specs=rows_spec, check_vma=False)
```

```python
import functools

import jax
import jax.numpy as jnp
from jax import lax
from jax.experimental import pallas as pl
from jax.experimental.pallas import tpu as pltpu
from jax.sharding import PartitionSpec as P

HEAD = 128
EPS = 1e-6
ROPE_BASE = 10000.0
F32, BF = jnp.float32, jnp.bfloat16


def _rms(x, w):
    xf = x.astype(F32)
    r = lax.rsqrt(jnp.mean(xf * xf, axis=-1, keepdims=True) + EPS)
    return (xf * r * w.astype(F32).reshape(1, -1)).astype(BF)


def _dot(a, b):
    return jnp.dot(a, b, preferred_element_type=F32)


MESH = pl.DeviceIdType.MESH


def _peer(me, r):
    p = me
    if r & 1:
        p = p + 1 - 2 * (me % 2)
    if r & 2:
        p = p + 2 - 4 * ((me // 2) % 2)
    if r & 4:
        p = p + 4 - 8 * (me // 4)
    return p


def _barrier(me, rels):
    sem = pltpu.get_barrier_semaphore()
    for r in rels:
        pl.semaphore_signal(sem, inc=1, device_id={'ep': _peer(me, r)}, device_id_type=MESH)
    return lambda: pl.semaphore_wait(sem, len(rels))


class _Tiles:
    def __init__(self, hbm, vmem, sems, first, count):
        self.hbm, self.vmem, self.sems, self.first, self.count = hbm, vmem, sems, first, count

    def copies(self, k):
        slot = lax.rem(k, 2)
        ft = self.vmem[0].shape[-1]
        part = pl.ds(pl.multiple_of((self.first + k) * ft, ft), ft)
        w1, w3, w2 = self.hbm
        src = (w1.at[:, part], w3.at[:, part], w2.at[part])
        return [pltpu.make_async_copy(a, b.at[slot], c.at[slot]) for a, b, c in zip(src, self.vmem, self.sems)]

    def start(self, k):
        for c in self.copies(k):
            c.start()

    def add(self, k, z, acc_ref):
        for c in self.copies(k):
            c.wait()
        slot = lax.rem(k, 2)
        acc_ref[...] += _ffn_tile(z, *(v[slot] for v in self.vmem))

        @pl.when(k + 2 < self.count)
        def _():
            self.start(k + 2)


def _tile_scratch(d, ft):
    dma = pltpu.SemaphoreType.DMA
    return [pltpu.VMEM((2, d, ft), BF), pltpu.VMEM((2, d, ft), BF), pltpu.VMEM((2, ft, d), BF), dma((2,)), dma((2,)), dma((2,))]


def _ffn_tile(z, w1, w3, w2):
    h1 = _dot(z, w1)
    h3 = _dot(z, w3)
    hid = (h1 * jax.nn.sigmoid(h1) * h3).astype(BF)
    return _dot(hid, w2)


def _first_kernel(h_ref, na_ref, nm_ref, nf_ref, wr_ref, idx_ref, cos_ref, sin_ref, wq_ref, wk_ref, wv_ref, wo_ref,
                  w1_hbm, w3_hbm, w2_hbm, z_ref, f_ref, uall_ref, gall_ref,
                  x_sc, acc_sc, u_sc, g_sc, sa, ra, sb, rb, sc, rc, sg, rg, ls, t1, t3, t2, q1, q3, q2s,
                  *, na_steps, nf_steps, hps, el, step_b, step_c):
    i = pl.program_id(0)
    t, d = h_ref.shape
    me = lax.axis_index('ep')
    hops = (1, 2, 4)
    half = t // 2
    tiles = _Tiles((w1_hbm, w3_hbm, w2_hbm), (t1, t3, t2), (q1, q3, q2s), 0, nf_steps)

    def remote(src, dst, s, r, rel):
        return pltpu.make_async_remote_copy(src_ref=src, dst_ref=dst, send_sem=s, recv_sem=r,
                                            device_id={'ep': _peer(me, rel)}, device_id_type=MESH)

    sends_a = ((1, 0, t), (2, 0, half), (4, half, half), (2, half, half), (4, 0, half))

    def stage_a(n):
        rel, start, size = sends_a[n]
        rows = pl.ds(start, size)
        return remote(u_sc.at[rows], uall_ref.at[rel, rows], sa.at[n], ra.at[n], rel)

    def stage_g(r):
        rows = pl.ds(pl.multiple_of(_peer(me, r) * el, el), el)
        return remote(g_sc.at[rows], gall_ref.at[r], sg.at[r - 1], rg.at[r - 1], r)

    def stage_b(n):
        rows = pl.ds(n * half, half)
        return remote(uall_ref.at[(2, 4)[n], rows], uall_ref.at[6, rows], sb.at[n], rb.at[n], (4, 2)[n])

    def stage_c(n):
        return remote(uall_ref.at[2 * n + 2], uall_ref.at[2 * n + 3], sc.at[n], rc.at[n], 1)

    def own():
        rows = pl.ds(pl.multiple_of(me * el, el), el)
        return (pltpu.make_async_copy(u_sc, uall_ref.at[0], ls.at[0]),
                pltpu.make_async_copy(g_sc.at[rows], gall_ref.at[0], ls.at[1]))

    @pl.when(i == 0)
    def _():
        arrived = _barrier(me, range(1, 8))
        u = _rms(h_ref[...], nm_ref[...])
        u_sc[...] = u
        logits = lax.dot_general(wr_ref[...], u, (((1,), (1,)), ((), ())), preferred_element_type=F32)
        row = lax.broadcasted_iota(jnp.int32, logits.shape, 0)
        routed = row == idx_ref[0:1, :]
        for j in range(1, idx_ref.shape[0]):
            routed = routed | (row == idx_ref[j:j + 1, :])
        lg = jnp.where(routed, logits, -jnp.inf)
        ex = jnp.exp(lg - jnp.max(lg, axis=0, keepdims=True))
        g_sc[...] = jnp.where(routed, ex / jnp.sum(ex, axis=0, keepdims=True), -1.0)
        arrived()
        for n in (1, 2, 3, 4, 0):
            stage_a(n).start()
        for r in range(1, 8):
            stage_g(r).start()
        for c in own():
            c.start()
        x_sc[...] = _rms(h_ref[...], na_ref[...])
        acc_sc[...] = jnp.zeros_like(acc_sc)

    @pl.when(i < na_steps)
    def _():
        x = x_sc[...]
        q2 = _dot(x, wq_ref[...])
        k2 = _dot(x, wk_ref[...])
        v2 = _dot(x, wv_ref[...]).astype(BF)
        cos, sin = cos_ref[...], sin_ref[...]
        causal = lax.broadcasted_iota(jnp.int32, (t, t), 0) >= lax.broadcasted_iota(jnp.int32, (t, t), 1)
        outs = []
        for h in range(hps):
            sl = slice(h * HEAD, (h + 1) * HEAD)
            q, k, v = q2[:, sl], k2[:, sl], v2[:, sl]
            q = (q * cos + pltpu.roll(q, HEAD // 2, 1) * sin).astype(BF)
            k = (k * cos + pltpu.roll(k, HEAD // 2, 1) * sin).astype(BF)
            s = lax.dot_general(q, k, (((1,), (1,)), ((), ())), preferred_element_type=F32) * HEAD ** -0.5
            s = jnp.where(causal, s, -jnp.inf)
            p = jnp.exp(s - jnp.max(s, axis=-1, keepdims=True))
            p = (p / jnp.sum(p, axis=-1, keepdims=True)).astype(BF)
            outs.append(_dot(p, v).astype(BF))
        acc_sc[...] += _dot(jnp.concatenate(outs, axis=1), wo_ref[...])

    @pl.when(i == na_steps - 1)
    def _():
        a = (h_ref[...].astype(F32) + acc_sc[...]).astype(BF)
        f_ref[...] = a.astype(F32)
        z_ref[...] = _rms(a, nf_ref[...])

    @pl.when(i == step_b)
    def _():
        for n in range(2):
            stage_a(n + 1).wait_recv()
            stage_b(n).start()

    @pl.when(i == na_steps)
    def _():
        for n in range(2):
            stage_a(n + 3).wait_recv()
            stage_c(n).start()

    @pl.when(i == step_c)
    def _():
        for n in range(2):
            stage_b(n).wait_recv()
        stage_c(2).start()

    @pl.when(i == na_steps - 3)
    def _():
        tiles.start(0)
        tiles.start(1)

    @pl.when((i >= na_steps) & (i < na_steps + nf_steps))
    def _():
        tiles.add(i - na_steps, z_ref[...], f_ref)

    @pl.when(i == na_steps + nf_steps)
    def _():
        stage_a(0).wait_recv()
        for n in range(5):
            stage_a(n).wait_send()
        for n in range(2):
            stage_b(n).wait_send()
        for n in range(3):
            stage_c(n).wait()
        for r in range(1, 8):
            stage_g(r).wait()
        for c in own():
            c.wait()


def _first(h, na, nm, nf, wr, idx, wq, wk, wv, wo, w1, w3, w2, el, nf_steps, ft):
    t, d = h.shape
    hps = 2
    w = HEAD * hps
    na_steps = wq.shape[1] // w
    ne = wr.shape[0]
    pos = jnp.arange(t).astype(F32)
    inv = ROPE_BASE ** (-2.0 * jnp.arange(HEAD // 2).astype(F32) / HEAD)
    ang = pos[:, None] * inv[None, :]
    c, s = jnp.cos(ang), jnp.sin(ang)
    cos, sin = jnp.concatenate([c, c], 1), jnp.concatenate([-s, s], 1)
    full = lambda shape: pl.BlockSpec(shape, lambda i: (0, 0))
    vec = pl.BlockSpec((d,), lambda i: (0,))
    ai = lambda i: jnp.minimum(i, na_steps - 1)
    any_ = pl.BlockSpec(memory_space=pl.ANY)
    dma = pltpu.SemaphoreType.DMA
    return pl.pallas_call(
        functools.partial(_first_kernel, na_steps=na_steps, nf_steps=nf_steps, hps=hps, el=el, step_b=na_steps - 2,
                          step_c=na_steps + nf_steps),
        grid=(na_steps + nf_steps + 1,),
        in_specs=[full((t, d)), vec, vec, vec, full((ne, d)), full(idx.shape),
                  full((t, HEAD)), full((t, HEAD))]
        + [pl.BlockSpec((d, w), lambda i: (0, ai(i)))] * 3
        + [pl.BlockSpec((w, d), lambda i: (ai(i), 0))]
        + [any_] * 3,
        out_specs=[full((t, d)), full((t, d)), any_, any_],
        out_shape=[jax.ShapeDtypeStruct((t, d), BF), jax.ShapeDtypeStruct((t, d), F32),
                   jax.ShapeDtypeStruct((8, t, d), BF), jax.ShapeDtypeStruct((8, el, t), F32)],
        scratch_shapes=[pltpu.VMEM((t, d), BF), pltpu.VMEM((t, d), F32), pltpu.VMEM((t, d), BF),
                        pltpu.VMEM((ne, t), F32),
                        dma((5,)), dma((5,)), dma((2,)), dma((2,)), dma((3,)), dma((3,)), dma((7,)), dma((7,)), dma((2,))] + _tile_scratch(d, ft),
        cost_estimate=pl.CostEstimate(flops=8 * t * d * d, bytes_accessed=8 * d * d, transcendentals=0),
        compiler_params=pltpu.CompilerParams(dimension_semantics=("arbitrary",), collective_id=0, has_side_effects=True,
                                             vmem_limit_bytes=56 << 20),
        name="first",
    )(h, na, nm, nf, wr, idx, cos, sin, wq, wk, wv, wo, w1, w3, w2)


def _hid_kernel(off_ref, nb_ref, g_ref, u_hbm, w1_hbm, w3_hbm, hid_hbm, gm_hbm,
                u_sc, x_sc, w1_sc, w3_sc, h_sc, hx_sc, gm_sc, su, sw1, sw3, sh, sg, *, ns, el, cap, nf, mb, depth):
    t, d = u_sc.shape[1:]
    ft = w1_sc.shape[-1]
    rows = ns * cap
    total = el * nf

    def fetch(k):
        slot = lax.rem(k, depth)
        e, f = lax.div(k, nf), lax.rem(k, nf)
        cols = pl.ds(pl.multiple_of(f * ft, ft), ft)
        return (pltpu.make_async_copy(w1_hbm.at[e, :, cols], w1_sc.at[slot], sw1.at[slot]),
                pltpu.make_async_copy(w3_hbm.at[e, :, cols], w3_sc.at[slot], sw3.at[slot]))

    def put_h(k):
        slot = lax.rem(k, 2)
        e, f = lax.div(k, nf), lax.rem(k, nf)
        cols = pl.ds(pl.multiple_of(f * ft, ft), ft)
        return pltpu.make_async_copy(hx_sc.at[slot], hid_hbm.at[e, :, cols], sh.at[slot])

    def put_g(s):
        slot = lax.rem(s, 2)
        return pltpu.make_async_copy(gm_sc.at[slot], gm_hbm.at[s], sg.at[slot])

    def get_u(s):
        return pltpu.make_async_copy(u_hbm.at[s], u_sc.at[s], su.at[s])

    for s in range(ns):
        get_u(s).start()
    for k in range(depth):
        for c in fetch(k):
            c.start()
    h_sc[...] = jnp.zeros_like(h_sc)
    it = lax.broadcasted_iota(jnp.int32, (cap, t), 0).astype(F32)
    before = jnp.where(lax.broadcasted_iota(jnp.int32, (t, t), 0) < lax.broadcasted_iota(jnp.int32, (t, t), 1), 1.0, 0.0)

    @pl.loop(0, ns)
    def _(s):
        g = g_ref[s]
        rank = jnp.where(g >= 0, _dot(jnp.where(g >= 0, 1.0, 0.0), before), -1.0)
        hit = [it == rank[e:e + 1, :] for e in range(el)]
        p = jnp.concatenate([jnp.where(h, 1.0, 0.0).astype(BF) for h in hit], axis=0)
        gt = jnp.concatenate([jnp.where(h, g[e:e + 1, :], 0.0) for e, h in enumerate(hit)], axis=0)
        gm = jnp.transpose(gt)
        ghi = gm.astype(BF)
        r1 = gm - ghi.astype(F32)
        gmid = r1.astype(BF)
        glo = (r1 - gmid.astype(F32)).astype(BF)

        @pl.when(s >= 2)
        def _():
            put_g(s - 2).wait()
        gm_sc[lax.rem(s, 2)] = jnp.concatenate([ghi, gmid, glo], axis=1)
        put_g(s).start()
        get_u(s).wait()
        for c in range(d // 512):
            cs = slice(c * 512, (c + 1) * 512)
            xv = _dot(p, u_sc[s, :, cs]).astype(BF)
            for e in range(el):
                o = pl.multiple_of(off_ref[s * el + e], 16)
                x_sc[e, pl.ds(o, cap), cs] = xv[e * cap:(e + 1) * cap]

    @pl.loop(0, total)
    def _(k):
        slot = lax.rem(k, depth)
        e = lax.div(k, nf)
        for c in fetch(k):
            c.wait()
        for m in range(mb, rows + 1, mb):
            @pl.when(nb_ref[e] == m // mb)
            def _():
                x = x_sc[e, :m, :]
                h1 = _dot(x, w1_sc[slot])
                h3 = _dot(x, w3_sc[slot])
                h_sc[:m, :] = (h1 * jax.nn.sigmoid(h1) * h3).astype(BF)

        @pl.when(k + depth < total)
        def _():
            for c in fetch(k + depth):
                c.start()

        @pl.when(k >= 2)
        def _():
            put_h(k - 2).wait()
        for s in range(ns):
            o = pl.multiple_of(off_ref[s * el + e], 16)
            hx_sc[lax.rem(k, 2), s * cap:(s + 1) * cap, :] = h_sc[pl.ds(o, cap), :]
        put_h(k).start()

    for s in (ns - 2, ns - 1):
        put_g(s).wait()
    for k in (total - 2, total - 1):
        put_h(k).wait()


def _hidden(u_all, g_all, ue1, ue3, cap):
    ns, t, d = u_all.shape
    el, _, fe = ue1.shape
    mb, nf, depth = 128, 2, 4
    ft = fe // nf
    cnt = jnp.sum((g_all >= 0).astype(jnp.int32), axis=-1)
    pad = (cnt + 15) // 16 * 16
    off = jnp.cumsum(pad, axis=0) - pad
    nb = jnp.maximum((jnp.sum(pad, axis=0) + mb - 1) // mb, 1)
    smem, vmem, any_ = (pl.BlockSpec(memory_space=m) for m in (pltpu.SMEM, pltpu.VMEM, pl.ANY))
    dma = pltpu.SemaphoreType.DMA
    return pl.pallas_call(
        functools.partial(_hid_kernel, ns=ns, el=el, cap=cap, nf=nf, mb=mb, depth=depth),
        in_specs=[smem, smem, vmem, any_, any_, any_],
        out_specs=[any_, any_],
        out_shape=[jax.ShapeDtypeStruct((el, ns * cap, fe), BF), jax.ShapeDtypeStruct((ns, t, 3 * el * cap), BF)],
        scratch_shapes=[pltpu.VMEM((ns, t, d), BF), pltpu.VMEM((el, ns * cap, d), BF), pltpu.VMEM((depth, d, ft), BF),
                        pltpu.VMEM((depth, d, ft), BF), pltpu.VMEM((ns * cap, ft), BF), pltpu.VMEM((2, ns * cap, ft), BF),
                        pltpu.VMEM((2, t, 3 * el * cap), BF),
                        dma((ns,)), dma((depth,)), dma((depth,)), dma((2,)), dma((2,))],
        cost_estimate=pl.CostEstimate(flops=4 * el * ns * cap * d * fe, bytes_accessed=4 * el * d * fe, transcendentals=0),
        compiler_params=pltpu.CompilerParams(vmem_limit_bytes=58 << 20),
        name="hidden",
    )(off.reshape(-1), nb, g_all, u_all, ue1, ue3)


E0 = {q: q + 1 for q in range(8)}
E1 = {0: 2, 1: 3, 2: 5, 3: 6, 4: 7, 5: 9, 6: 12, 7: 15}
E2 = {0: 8, 1: 8, 2: 11, 3: 12, 4: 14, 5: 16, 6: 16, 7: 16}
NQ, F_FROM, STEPS = 8, 4, 17


def _last_kernel(hid_hbm, gm_hbm, z_hbm, f_hbm, ue2_ref, w1_hbm, w3_hbm, w2_hbm, o_ref,
                 hid_sc, gm_sc, z_ref, y_sc, keep_sc, ps_sc, r0_sc, r1_sc, r2_sc, acc_sc, hs, gs, zs, s0, r0, s1, r1, s2, r2,
                 t1, t3, t2, q1, q3, q2s, *, ns, el, cap, f0, nfs):
    i = pl.program_id(0)
    t, d = z_ref.shape
    half = t // 2
    cw = ue2_ref.shape[-1]
    me = lax.axis_index('ep')
    tiles = _Tiles((w1_hbm, w3_hbm, w2_hbm), (t1, t3, t2), (q1, q3, q2s), f0, nfs)

    def get_h(e):
        return pltpu.make_async_copy(hid_hbm.at[e], hid_sc.at[e], hs.at[e])

    def get_g(s):
        return pltpu.make_async_copy(gm_hbm.at[s], gm_sc.at[s], gs.at[s])

    def remote(src, dst, s, r, dev):
        return pltpu.make_async_remote_copy(src_ref=src, dst_ref=dst, send_sem=s, recv_sem=r,
                                            device_id={'ep': dev}, device_id_type=MESH)

    def get_zf():
        return (pltpu.make_async_copy(z_hbm, z_ref, zs.at[0]), pltpu.make_async_copy(f_hbm, acc_sc, zs.at[1]))

    def send0(q, slot):
        return remote(ps_sc.at[slot], r0_sc.at[q], s0.at[q], r0.at[q], _peer(me, 1))

    def send1(q, h):
        return remote(r0_sc.at[q, h, pl.ds(2, 2)], r1_sc.at[q, h], s1.at[2 * q + h], r1.at[2 * q + h], _peer(me, (2, 4)[h]))

    def send2(q, h):
        return remote(r0_sc.at[q, h, 1], r2_sc.at[q, h], s2.at[2 * q + h], r2.at[2 * q + h], _peer(me, (4, 2)[h]))

    @pl.when(i == 0)
    def _():
        arrived = _barrier(me, (1, 2, 4))
        for e in range(el):
            get_h(e).start()
        for s in range(ns):
            get_g(s).start()
        for c in get_zf():
            c.start()
        arrived()
        for e in range(el):
            get_h(e).wait()

    def pass_on(qs):
        for q in qs:
            @pl.when(i == E0[q])
            def _():
                send0(q, q % 2).wait_recv()
                r0_sc[q] += keep_sc[...]
                for h in range(2):
                    send1(q, h).start()

    pass_on((0, 1))

    @pl.when(i < NQ)
    def _():
        for e in range(el):
            y = _dot(hid_sc[e], ue2_ref[e]).astype(BF)
            for s in range(ns):
                y_sc[s, e * cap:(e + 1) * cap, :] = y[s * cap:(s + 1) * cap]

    pass_on(range(2, NQ))

    @pl.when(i == 0)
    def _():
        for s in range(ns):
            get_g(s).wait()
        tiles.start(0)
        tiles.start(1)

    @pl.when((i >= 2) & (i < NQ))
    def _():
        send0(i - 2, i % 2).wait_send()

    @pl.when(i < NQ)
    def _():
        kk = el * cap
        for b in range(4):
            for c in range(2):
                s = 2 * b + c
                y = y_sc[s]
                m = _dot(gm_sc[s, :, :kk], y) + _dot(gm_sc[s, :, kk:2 * kk], y) + _dot(gm_sc[s, :, 2 * kk:], y)
                for h, pos in enumerate(((0, 2, 1, 3)[b], b)):
                    part = m[h * half:(h + 1) * half]
                    if c == 0:
                        keep_sc[h, pos] = part
                    else:
                        ps_sc[i % 2, h, pos] = part
        send0(i, i % 2).start()

    @pl.when(i == F_FROM)
    def _():
        for c in get_zf():
            c.wait()

    @pl.when((i >= F_FROM) & (i < F_FROM + nfs))
    def _():
        tiles.add(i - F_FROM, z_ref[...], acc_sc)

    for q, step in E1.items():
        @pl.when(i == step)
        def _():
            for h in range(2):
                send1(q, h).wait_recv()
                r0_sc[q, h, 0:2] += r1_sc[q, h]
                send2(q, h).start()

    for q, step in E2.items():
        @pl.when(i == step)
        def _():
            for h in range(2):
                send2(q, h).wait_recv()
                acc_sc[h * half:(h + 1) * half, q * cw:(q + 1) * cw] += r0_sc[q, h, 0] + r2_sc[q, h]

    @pl.when(i == STEPS - 1)
    def _():
        for q in (NQ - 2, NQ - 1):
            send0(q, q % 2).wait_send()
        for q in range(NQ):
            for h in range(2):
                send1(q, h).wait_send()
                send2(q, h).wait_send()
        o_ref[...] = acc_sc[...].astype(BF)


def _last(hid, gm, z, f, ue2, w1, w3, w2, cap, ft, f0):
    t, d = z.shape
    el, rows, fe = hid.shape
    ns = rows // cap
    cw = d // NQ
    nfs = w1.shape[1] // ft - f0
    full = lambda shape: pl.BlockSpec(shape, lambda i: (0, 0), pipeline_mode=pl.Buffered(1))
    qi = lambda i: jnp.minimum(i, NQ - 1)
    any_ = pl.BlockSpec(memory_space=pl.ANY)
    dma = pltpu.SemaphoreType.DMA
    return pl.pallas_call(
        functools.partial(_last_kernel, ns=ns, el=el, cap=cap, f0=f0, nfs=nfs),
        grid=(STEPS,),
        in_specs=[any_, any_, any_, any_,
                  pl.BlockSpec((el, fe, cw), lambda i: (0, 0, qi(i)))] + [any_] * 3,
        out_specs=full((t, d)),
        out_shape=jax.ShapeDtypeStruct((t, d), BF),
        scratch_shapes=[pltpu.VMEM((el, rows, fe), BF), pltpu.VMEM(gm.shape, BF), pltpu.VMEM((t, d), BF),
                        pltpu.VMEM((ns, el * cap, cw), BF),
                        pltpu.VMEM((2, 4, t // 2, cw), F32), pltpu.VMEM((2, 2, 4, t // 2, cw), F32),
                        pltpu.VMEM((NQ, 2, 4, t // 2, cw), F32), pltpu.VMEM((NQ, 2, 2, t // 2, cw), F32),
                        pltpu.VMEM((NQ, 2, t // 2, cw), F32), pltpu.VMEM((t, d), F32),
                        dma((el,)), dma((ns,)), dma((2,))] + [dma((NQ,))] * 2 + [dma((2 * NQ,))] * 4 + _tile_scratch(d, ft),
        cost_estimate=pl.CostEstimate(flops=2 * el * rows * d * fe, bytes_accessed=2 * el * d * fe, transcendentals=0),
        compiler_params=pltpu.CompilerParams(dimension_semantics=("arbitrary",), collective_id=1, has_side_effects=True,
                                             vmem_limit_bytes=67043328),
        name="last",
    )(hid, gm, z, f, ue2, w1, w3, w2)


def solution(mesh):
    G = mesh.shape['ep']
    ft, f0 = 512, 4

    def local(h0, idx, slot, na, wq, wk, wv, wo, nf, w1, w3, w2, nm, wr, ue1, ue3, ue2):
        b, s, d = h0.shape
        t = b * s
        k = idx.shape[-1]
        el = ue1.shape[0]
        cap = 2 * t * k // (el * G)
        z, f, u_all, g_all = _first(h0.reshape(t, d), na, nm, nf, wr.T, idx.reshape(t, k).T, wq, wk, wv, wo, w1, w3, w2,
                                    el, f0, ft)
        hid, gm = _hidden(u_all, g_all, ue1, ue3, cap)
        return _last(hid, gm, z, f, ue2, w1, w3, w2, cap, ft, f0).reshape(b, s, d)

    rows_spec = P(('dp', 'ep'))
    in_specs = (rows_spec,) * 3 + (P(),) * 11 + (P('ep'),) * 3
    return jax.shard_map(local, mesh=mesh, in_specs=in_specs, out_specs=rows_spec, check_vma=False)
```

```python
import functools

import jax
import jax.numpy as jnp
from jax import lax
from jax.experimental import pallas as pl
from jax.experimental.pallas import tpu as pltpu
from jax.sharding import PartitionSpec as P

HEAD = 128
EPS = 1e-6
ROPE_BASE = 10000.0
F32, BF = jnp.float32, jnp.bfloat16


def _rms(x, w):
    xf = x.astype(F32)
    r = lax.rsqrt(jnp.mean(xf * xf, axis=-1, keepdims=True) + EPS)
    return (xf * r * w.astype(F32).reshape(1, -1)).astype(BF)


def _dot(a, b):
    return jnp.dot(a, b, preferred_element_type=F32)


MESH = pl.DeviceIdType.MESH
MB = 128


def _peer(me, r):
    p = me
    if r & 1:
        p = p + 1 - 2 * (me % 2)
    if r & 2:
        p = p + 2 - 4 * ((me // 2) % 2)
    if r & 4:
        p = p + 4 - 8 * (me // 4)
    return p


def _barrier(me, rels):
    sem = pltpu.get_barrier_semaphore()
    for r in rels:
        pl.semaphore_signal(sem, inc=1, device_id={'ep': _peer(me, r)}, device_id_type=MESH)
    return lambda: pl.semaphore_wait(sem, len(rels))


class _Tiles:
    def __init__(self, hbm, vmem, sems, first, count):
        self.hbm, self.vmem, self.sems, self.first, self.count = hbm, vmem, sems, first, count

    def copies(self, k):
        slot = lax.rem(k, 2)
        ft = self.vmem[0].shape[-1]
        part = pl.ds(pl.multiple_of((self.first + k) * ft, ft), ft)
        w1, w3, w2 = self.hbm
        src = (w1.at[:, part], w3.at[:, part], w2.at[part])
        return [pltpu.make_async_copy(a, b.at[slot], c.at[slot]) for a, b, c in zip(src, self.vmem, self.sems)]

    def start(self, k):
        for c in self.copies(k):
            c.start()

    def add(self, k, z, acc_ref):
        for c in self.copies(k):
            c.wait()
        slot = lax.rem(k, 2)
        acc_ref[...] += _ffn_tile(z, *(v[slot] for v in self.vmem))

        @pl.when(k + 2 < self.count)
        def _():
            self.start(k + 2)


def _tile_scratch(d, ft):
    dma = pltpu.SemaphoreType.DMA
    return [pltpu.VMEM((2, d, ft), BF), pltpu.VMEM((2, d, ft), BF), pltpu.VMEM((2, ft, d), BF), dma((2,)), dma((2,)), dma((2,))]


def _ffn_tile(z, w1, w3, w2):
    h1 = _dot(z, w1)
    h3 = _dot(z, w3)
    hid = (h1 * jax.nn.sigmoid(h1) * h3).astype(BF)
    return _dot(hid, w2)


def _first_kernel(h_ref, na_ref, nm_ref, nf_ref, wr_ref, idx_ref, cos_ref, sin_ref, wq_ref, wk_ref, wv_ref, wo_ref,
                  w1_hbm, w3_hbm, w2_hbm, z_ref, f_ref, uall_ref, gall_ref, off_ref,
                  x_sc, acc_sc, u_sc, g_sc, gv_sc, sa, ra, sb, rb, sc, rc, sg, rg, ls, lg, t1, t3, t2, q1, q3, q2s,
                  *, na_steps, nf_steps, hps, el, step_b, step_c):
    i = pl.program_id(0)
    t, d = h_ref.shape
    me = lax.axis_index('ep')
    hops = (1, 2, 4)
    half = t // 2
    tiles = _Tiles((w1_hbm, w3_hbm, w2_hbm), (t1, t3, t2), (q1, q3, q2s), 0, nf_steps)

    def remote(src, dst, s, r, rel):
        return pltpu.make_async_remote_copy(src_ref=src, dst_ref=dst, send_sem=s, recv_sem=r,
                                            device_id={'ep': _peer(me, rel)}, device_id_type=MESH)

    sends_a = ((1, 0, t), (2, 0, half), (4, half, half), (2, half, half), (4, 0, half))

    def stage_a(n):
        rel, start, size = sends_a[n]
        rows = pl.ds(start, size)
        return remote(u_sc.at[rows], uall_ref.at[rel, rows], sa.at[n], ra.at[n], rel)

    def stage_g(r):
        rows = pl.ds(pl.multiple_of(_peer(me, r) * el, el), el)
        return remote(g_sc.at[rows], gall_ref.at[r], sg.at[r - 1], rg.at[r - 1], r)

    def stage_b(n):
        rows = pl.ds(n * half, half)
        return remote(uall_ref.at[(2, 4)[n], rows], uall_ref.at[6, rows], sb.at[n], rb.at[n], (4, 2)[n])

    def stage_c(n):
        return remote(uall_ref.at[2 * n + 2], uall_ref.at[2 * n + 3], sc.at[n], rc.at[n], 1)

    def own():
        rows = pl.ds(pl.multiple_of(me * el, el), el)
        return (pltpu.make_async_copy(u_sc, uall_ref.at[0], ls.at[0]),
                pltpu.make_async_copy(g_sc.at[rows], gall_ref.at[0], ls.at[1]))

    @pl.when(i == 0)
    def _():
        arrived = _barrier(me, range(1, 8))
        u = _rms(h_ref[...], nm_ref[...])
        u_sc[...] = u
        logits = lax.dot_general(wr_ref[...], u, (((1,), (1,)), ((), ())), preferred_element_type=F32)
        row = lax.broadcasted_iota(jnp.int32, logits.shape, 0)
        routed = row == idx_ref[0:1, :]
        for j in range(1, idx_ref.shape[0]):
            routed = routed | (row == idx_ref[j:j + 1, :])
        lg = jnp.where(routed, logits, -jnp.inf)
        ex = jnp.exp(lg - jnp.max(lg, axis=0, keepdims=True))
        g_sc[...] = jnp.where(routed, ex / jnp.sum(ex, axis=0, keepdims=True), -1.0)
        arrived()
        for n in (1, 2, 3, 4, 0):
            stage_a(n).start()
        for r in range(1, 8):
            stage_g(r).start()
        for c in own():
            c.start()
        x_sc[...] = _rms(h_ref[...], na_ref[...])
        acc_sc[...] = jnp.zeros_like(acc_sc)

    @pl.when(i < na_steps)
    def _():
        x = x_sc[...]
        q2 = _dot(x, wq_ref[...])
        k2 = _dot(x, wk_ref[...])
        v2 = _dot(x, wv_ref[...]).astype(BF)
        cos, sin = cos_ref[...], sin_ref[...]
        causal = lax.broadcasted_iota(jnp.int32, (t, t), 0) >= lax.broadcasted_iota(jnp.int32, (t, t), 1)
        outs = []
        for h in range(hps):
            sl = slice(h * HEAD, (h + 1) * HEAD)
            q, k, v = q2[:, sl], k2[:, sl], v2[:, sl]
            q = (q * cos + pltpu.roll(q, HEAD // 2, 1) * sin).astype(BF)
            k = (k * cos + pltpu.roll(k, HEAD // 2, 1) * sin).astype(BF)
            s = lax.dot_general(q, k, (((1,), (1,)), ((), ())), preferred_element_type=F32) * HEAD ** -0.5
            s = jnp.where(causal, s, -jnp.inf)
            p = jnp.exp(s - jnp.max(s, axis=-1, keepdims=True))
            p = (p / jnp.sum(p, axis=-1, keepdims=True)).astype(BF)
            outs.append(_dot(p, v).astype(BF))
        acc_sc[...] += _dot(jnp.concatenate(outs, axis=1), wo_ref[...])

    @pl.when(i == na_steps - 1)
    def _():
        a = (h_ref[...].astype(F32) + acc_sc[...]).astype(BF)
        f_ref[...] = a.astype(F32)
        z_ref[...] = _rms(a, nf_ref[...])

    @pl.when(i == step_b)
    def _():
        for n in range(2):
            stage_a(n + 1).wait_recv()
            stage_b(n).start()

    @pl.when(i == na_steps)
    def _():
        for n in range(2):
            stage_a(n + 3).wait_recv()
            stage_c(n).start()

    @pl.when(i == step_c)
    def _():
        for n in range(2):
            stage_b(n).wait_recv()
        stage_c(2).start()

    @pl.when(i == na_steps - 3)
    def _():
        tiles.start(0)
        tiles.start(1)

    @pl.when((i >= na_steps) & (i < na_steps + nf_steps))
    def _():
        tiles.add(i - na_steps, z_ref[...], f_ref)

    @pl.when(i == na_steps + nf_steps)
    def _():
        stage_a(0).wait_recv()
        for n in range(5):
            stage_a(n).wait_send()
        for n in range(2):
            stage_b(n).wait_send()
        for n in range(3):
            stage_c(n).wait()
        own()[0].wait()

    @pl.when(i == na_steps + 1)
    def _():
        for r in range(1, 8):
            stage_g(r).wait()
        own()[1].wait()
        back = pltpu.make_async_copy(gall_ref, gv_sc, lg.at[0])
        back.start()
        back.wait()
        base = jnp.zeros((el, 1), jnp.int32)
        for r in range(8):
            off_ref[r] = jnp.broadcast_to(base, (el, 128))
            cnt = jnp.sum(jnp.where(gv_sc[r] >= 0, 1.0, 0.0), axis=1, keepdims=True).astype(jnp.int32)
            base = base + (cnt + 15) // 16 * 16
        off_ref[8] = jnp.broadcast_to(jnp.maximum((base + MB - 1) // MB, 1), (el, 128))


def _first(h, na, nm, nf, wr, idx, wq, wk, wv, wo, w1, w3, w2, el, nf_steps, ft):
    t, d = h.shape
    hps = 2
    w = HEAD * hps
    na_steps = wq.shape[1] // w
    ne = wr.shape[0]
    pos = jnp.arange(t).astype(F32)
    inv = ROPE_BASE ** (-2.0 * jnp.arange(HEAD // 2).astype(F32) / HEAD)
    ang = pos[:, None] * inv[None, :]
    c, s = jnp.cos(ang), jnp.sin(ang)
    cos, sin = jnp.concatenate([c, c], 1), jnp.concatenate([-s, s], 1)
    full = lambda shape: pl.BlockSpec(shape, lambda i: (0, 0))
    vec = pl.BlockSpec((d,), lambda i: (0,))
    ai = lambda i: jnp.minimum(i, na_steps - 1)
    any_ = pl.BlockSpec(memory_space=pl.ANY)
    dma = pltpu.SemaphoreType.DMA
    return pl.pallas_call(
        functools.partial(_first_kernel, na_steps=na_steps, nf_steps=nf_steps, hps=hps, el=el, step_b=na_steps - 2,
                          step_c=na_steps + nf_steps),
        grid=(na_steps + nf_steps + 1,),
        in_specs=[full((t, d)), vec, vec, vec, full((ne, d)), full(idx.shape),
                  full((t, HEAD)), full((t, HEAD))]
        + [pl.BlockSpec((d, w), lambda i: (0, ai(i)))] * 3
        + [pl.BlockSpec((w, d), lambda i: (ai(i), 0))]
        + [any_] * 3,
        out_specs=[full((t, d)), full((t, d)), any_, any_, pl.BlockSpec((9, el, 128), lambda i: (0, 0, 0))],
        out_shape=[jax.ShapeDtypeStruct((t, d), BF), jax.ShapeDtypeStruct((t, d), F32),
                   jax.ShapeDtypeStruct((8, t, d), BF), jax.ShapeDtypeStruct((8, el, t), F32),
                   jax.ShapeDtypeStruct((9, el, 128), jnp.int32)],
        scratch_shapes=[pltpu.VMEM((t, d), BF), pltpu.VMEM((t, d), F32), pltpu.VMEM((t, d), BF),
                        pltpu.VMEM((ne, t), F32), pltpu.VMEM((8, el, t), F32),
                        dma((5,)), dma((5,)), dma((2,)), dma((2,)), dma((3,)), dma((3,)), dma((7,)), dma((7,)), dma((2,)), dma((1,))] + _tile_scratch(d, ft),
        cost_estimate=pl.CostEstimate(flops=8 * t * d * d, bytes_accessed=8 * d * d, transcendentals=0),
        compiler_params=pltpu.CompilerParams(dimension_semantics=("arbitrary",), collective_id=0, has_side_effects=True,
                                             vmem_limit_bytes=56 << 20),
        name="first",
    )(h, na, nm, nf, wr, idx, cos, sin, wq, wk, wv, wo, w1, w3, w2)


def _hid_kernel(off_ref, g_ref, u_hbm, w1_hbm, w3_hbm, hid_hbm, gm_hbm,
                u_sc, x_sc, w1_sc, w3_sc, h_sc, hx_sc, gm_sc, su, sw1, sw3, sh, sg, *, ns, el, cap, nf, mb, depth):
    t, d = u_sc.shape[1:]
    ft = w1_sc.shape[-1]
    rows = ns * cap
    total = el * nf

    def fetch(k):
        slot = lax.rem(k, depth)
        e, f = lax.div(k, nf), lax.rem(k, nf)
        cols = pl.ds(pl.multiple_of(f * ft, ft), ft)
        return (pltpu.make_async_copy(w1_hbm.at[e, :, cols], w1_sc.at[slot], sw1.at[slot]),
                pltpu.make_async_copy(w3_hbm.at[e, :, cols], w3_sc.at[slot], sw3.at[slot]))

    def put_h(k):
        slot = lax.rem(k, 2)
        e, f = lax.div(k, nf), lax.rem(k, nf)
        cols = pl.ds(pl.multiple_of(f * ft, ft), ft)
        return pltpu.make_async_copy(hx_sc.at[slot], hid_hbm.at[e, :, cols], sh.at[slot])

    def put_g(s):
        slot = lax.rem(s, 2)
        return pltpu.make_async_copy(gm_sc.at[slot], gm_hbm.at[s], sg.at[slot])

    def get_u(s):
        return pltpu.make_async_copy(u_hbm.at[s], u_sc.at[s], su.at[s])

    for s in range(ns):
        get_u(s).start()
    for k in range(depth):
        for c in fetch(k):
            c.start()
    h_sc[...] = jnp.zeros_like(h_sc)
    it = lax.broadcasted_iota(jnp.int32, (cap, t), 0).astype(F32)
    before = jnp.where(lax.broadcasted_iota(jnp.int32, (t, t), 0) < lax.broadcasted_iota(jnp.int32, (t, t), 1), 1.0, 0.0)

    @pl.loop(0, ns)
    def _(s):
        g = g_ref[s]
        rank = jnp.where(g >= 0, _dot(jnp.where(g >= 0, 1.0, 0.0), before), -1.0)
        hit = [it == rank[e:e + 1, :] for e in range(el)]
        p = jnp.concatenate([jnp.where(h, 1.0, 0.0).astype(BF) for h in hit], axis=0)
        gt = jnp.concatenate([jnp.where(h, g[e:e + 1, :], 0.0) for e, h in enumerate(hit)], axis=0)
        gm = jnp.transpose(gt)
        ghi = gm.astype(BF)
        r1 = gm - ghi.astype(F32)
        gmid = r1.astype(BF)
        glo = (r1 - gmid.astype(F32)).astype(BF)

        @pl.when(s >= 2)
        def _():
            put_g(s - 2).wait()
        gm_sc[lax.rem(s, 2)] = jnp.concatenate([ghi, gmid, glo], axis=1)
        put_g(s).start()
        get_u(s).wait()
        for c in range(d // 512):
            cs = slice(c * 512, (c + 1) * 512)
            xv = _dot(p, u_sc[s, :, cs]).astype(BF)
            for e in range(el):
                o = pl.multiple_of(off_ref[s, e, 0], 16)
                x_sc[e, pl.ds(o, cap), cs] = xv[e * cap:(e + 1) * cap]

    @pl.loop(0, total)
    def _(k):
        slot = lax.rem(k, depth)
        e = lax.div(k, nf)
        for c in fetch(k):
            c.wait()
        for m in range(mb, rows + 1, mb):
            @pl.when(off_ref[ns, e, 0] == m // mb)
            def _():
                x = x_sc[e, :m, :]
                h1 = _dot(x, w1_sc[slot])
                h3 = _dot(x, w3_sc[slot])
                h_sc[:m, :] = (h1 * jax.nn.sigmoid(h1) * h3).astype(BF)

        @pl.when(k + depth < total)
        def _():
            for c in fetch(k + depth):
                c.start()

        @pl.when(k >= 2)
        def _():
            put_h(k - 2).wait()
        for s in range(ns):
            o = pl.multiple_of(off_ref[s, e, 0], 16)
            hx_sc[lax.rem(k, 2), s * cap:(s + 1) * cap, :] = h_sc[pl.ds(o, cap), :]
        put_h(k).start()

    for s in (ns - 2, ns - 1):
        put_g(s).wait()
    for k in (total - 2, total - 1):
        put_h(k).wait()


def _hidden(u_all, g_all, off, ue1, ue3, cap):
    ns, t, d = u_all.shape
    el, _, fe = ue1.shape
    mb, nf, depth = MB, 2, 4
    ft = fe // nf
    smem, vmem, any_ = (pl.BlockSpec(memory_space=m) for m in (pltpu.SMEM, pltpu.VMEM, pl.ANY))
    dma = pltpu.SemaphoreType.DMA
    return pl.pallas_call(
        functools.partial(_hid_kernel, ns=ns, el=el, cap=cap, nf=nf, mb=mb, depth=depth),
        in_specs=[smem, vmem, any_, any_, any_],
        out_specs=[any_, any_],
        out_shape=[jax.ShapeDtypeStruct((el, ns * cap, fe), BF), jax.ShapeDtypeStruct((ns, t, 3 * el * cap), BF)],
        scratch_shapes=[pltpu.VMEM((ns, t, d), BF), pltpu.VMEM((el, ns * cap, d), BF), pltpu.VMEM((depth, d, ft), BF),
                        pltpu.VMEM((depth, d, ft), BF), pltpu.VMEM((ns * cap, ft), BF), pltpu.VMEM((2, ns * cap, ft), BF),
                        pltpu.VMEM((2, t, 3 * el * cap), BF),
                        dma((ns,)), dma((depth,)), dma((depth,)), dma((2,)), dma((2,))],
        cost_estimate=pl.CostEstimate(flops=4 * el * ns * cap * d * fe, bytes_accessed=4 * el * d * fe, transcendentals=0),
        compiler_params=pltpu.CompilerParams(vmem_limit_bytes=58 << 20),
        name="hidden",
    )(off, g_all, u_all, ue1, ue3)


E0 = {q: q + 1 for q in range(8)}
E1 = {0: 2, 1: 3, 2: 5, 3: 6, 4: 7, 5: 9, 6: 12, 7: 15}
E2 = {0: 8, 1: 8, 2: 11, 3: 12, 4: 14, 5: 16, 6: 16, 7: 16}
NQ, F_FROM, STEPS = 8, 4, 17


def _last_kernel(hid_hbm, gm_hbm, z_hbm, f_hbm, ue2_ref, w1_hbm, w3_hbm, w2_hbm, o_ref,
                 hid_sc, gm_sc, z_ref, y_sc, keep_sc, ps_sc, r0_sc, r1_sc, r2_sc, acc_sc, hs, gs, zs, s0, r0, s1, r1, s2, r2,
                 t1, t3, t2, q1, q3, q2s, *, ns, el, cap, f0, nfs):
    i = pl.program_id(0)
    t, d = z_ref.shape
    half = t // 2
    cw = ue2_ref.shape[-1]
    me = lax.axis_index('ep')
    tiles = _Tiles((w1_hbm, w3_hbm, w2_hbm), (t1, t3, t2), (q1, q3, q2s), f0, nfs)

    def get_h(e):
        return pltpu.make_async_copy(hid_hbm.at[e], hid_sc.at[e], hs.at[e])

    def get_g(s):
        return pltpu.make_async_copy(gm_hbm.at[s], gm_sc.at[s], gs.at[s])

    def remote(src, dst, s, r, dev):
        return pltpu.make_async_remote_copy(src_ref=src, dst_ref=dst, send_sem=s, recv_sem=r,
                                            device_id={'ep': dev}, device_id_type=MESH)

    def get_zf():
        return (pltpu.make_async_copy(z_hbm, z_ref, zs.at[0]), pltpu.make_async_copy(f_hbm, acc_sc, zs.at[1]))

    def send0(q, slot):
        return remote(ps_sc.at[slot], r0_sc.at[q], s0.at[q], r0.at[q], _peer(me, 1))

    def send1(q, h):
        return remote(r0_sc.at[q, h, pl.ds(2, 2)], r1_sc.at[q, h], s1.at[2 * q + h], r1.at[2 * q + h], _peer(me, (2, 4)[h]))

    def send2(q, h):
        return remote(r0_sc.at[q, h, 1], r2_sc.at[q, h], s2.at[2 * q + h], r2.at[2 * q + h], _peer(me, (4, 2)[h]))

    @pl.when(i == 0)
    def _():
        arrived = _barrier(me, (1, 2, 4))
        for e in range(el):
            get_h(e).start()
        for s in range(ns):
            get_g(s).start()
        for c in get_zf():
            c.start()
        arrived()

    def pass_on(qs):
        for q in qs:
            @pl.when(i == E0[q])
            def _():
                send0(q, q % 2).wait_recv()
                r0_sc[q] += keep_sc[...]
                for h in range(2):
                    send1(q, h).start()

    pass_on((0, 1))

    def expert(e):
        y = _dot(hid_sc[e], ue2_ref[e]).astype(BF)
        for s in range(ns):
            y_sc[s, e * cap:(e + 1) * cap, :] = y[s * cap:(s + 1) * cap]

    @pl.when(i == 0)
    def _():
        for e in range(el):
            get_h(e).wait()
            expert(e)

    @pl.when((i > 0) & (i < NQ))
    def _():
        for e in range(el):
            expert(e)

    pass_on(range(2, NQ))

    @pl.when(i == 0)
    def _():
        for s in range(ns):
            get_g(s).wait()
        tiles.start(0)
        tiles.start(1)

    @pl.when((i >= 2) & (i < NQ))
    def _():
        send0(i - 2, i % 2).wait_send()

    @pl.when(i < NQ)
    def _():
        kk = el * cap
        for c in (1, 0):
            for b in range(4):
                s = 2 * b + c
                y = y_sc[s]
                m = _dot(gm_sc[s, :, :kk], y) + _dot(gm_sc[s, :, kk:2 * kk], y) + _dot(gm_sc[s, :, 2 * kk:], y)
                for h, pos in enumerate(((0, 2, 1, 3)[b], b)):
                    part = m[h * half:(h + 1) * half]
                    if c == 0:
                        keep_sc[h, pos] = part
                    else:
                        ps_sc[i % 2, h, pos] = part
            if c == 1:
                send0(i, i % 2).start()

    @pl.when(i == F_FROM)
    def _():
        for c in get_zf():
            c.wait()

    @pl.when((i >= F_FROM) & (i < F_FROM + nfs))
    def _():
        tiles.add(i - F_FROM, z_ref[...], acc_sc)

    for q, step in E1.items():
        @pl.when(i == step)
        def _():
            for h in range(2):
                send1(q, h).wait_recv()
                r0_sc[q, h, 0:2] += r1_sc[q, h]
                send2(q, h).start()

    for q, step in E2.items():
        @pl.when(i == step)
        def _():
            for h in range(2):
                send2(q, h).wait_recv()
                acc_sc[h * half:(h + 1) * half, q * cw:(q + 1) * cw] += r0_sc[q, h, 0] + r2_sc[q, h]

    @pl.when(i == STEPS - 1)
    def _():
        for q in (NQ - 2, NQ - 1):
            send0(q, q % 2).wait_send()
        for q in range(NQ):
            for h in range(2):
                send1(q, h).wait_send()
                send2(q, h).wait_send()
        o_ref[...] = acc_sc[...].astype(BF)


def _last(hid, gm, z, f, ue2, w1, w3, w2, cap, ft, f0):
    t, d = z.shape
    el, rows, fe = hid.shape
    ns = rows // cap
    cw = d // NQ
    nfs = w1.shape[1] // ft - f0
    full = lambda shape: pl.BlockSpec(shape, lambda i: (0, 0), pipeline_mode=pl.Buffered(1))
    qi = lambda i: jnp.minimum(i, NQ - 1)
    any_ = pl.BlockSpec(memory_space=pl.ANY)
    dma = pltpu.SemaphoreType.DMA
    return pl.pallas_call(
        functools.partial(_last_kernel, ns=ns, el=el, cap=cap, f0=f0, nfs=nfs),
        grid=(STEPS,),
        in_specs=[any_, any_, any_, any_,
                  pl.BlockSpec((el, fe, cw), lambda i: (0, 0, qi(i)))] + [any_] * 3,
        out_specs=full((t, d)),
        out_shape=jax.ShapeDtypeStruct((t, d), BF),
        scratch_shapes=[pltpu.VMEM((el, rows, fe), BF), pltpu.VMEM(gm.shape, BF), pltpu.VMEM((t, d), BF),
                        pltpu.VMEM((ns, el * cap, cw), BF),
                        pltpu.VMEM((2, 4, t // 2, cw), F32), pltpu.VMEM((2, 2, 4, t // 2, cw), F32),
                        pltpu.VMEM((NQ, 2, 4, t // 2, cw), F32), pltpu.VMEM((NQ, 2, 2, t // 2, cw), F32),
                        pltpu.VMEM((NQ, 2, t // 2, cw), F32), pltpu.VMEM((t, d), F32),
                        dma((el,)), dma((ns,)), dma((2,))] + [dma((NQ,))] * 2 + [dma((2 * NQ,))] * 4 + _tile_scratch(d, ft),
        cost_estimate=pl.CostEstimate(flops=2 * el * rows * d * fe, bytes_accessed=2 * el * d * fe, transcendentals=0),
        compiler_params=pltpu.CompilerParams(dimension_semantics=("arbitrary",), collective_id=1, has_side_effects=True,
                                             vmem_limit_bytes=67043328),
        name="last",
    )(hid, gm, z, f, ue2, w1, w3, w2)


def solution(mesh):
    G = mesh.shape['ep']
    ft, f0 = 512, 4

    def local(h0, idx, slot, na, wq, wk, wv, wo, nf, w1, w3, w2, nm, wr, ue1, ue3, ue2):
        b, s, d = h0.shape
        t = b * s
        k = idx.shape[-1]
        el = ue1.shape[0]
        cap = 2 * t * k // (el * G)
        z, f, u_all, g_all, off = _first(h0.reshape(t, d), na, nm, nf, wr.T, idx.reshape(t, k).T, wq, wk, wv, wo, w1, w3, w2,
                                    el, f0, ft)
        hid, gm = _hidden(u_all, g_all, off, ue1, ue3, cap)
        return _last(hid, gm, z, f, ue2, w1, w3, w2, cap, ft, f0).reshape(b, s, d)

    rows_spec = P(('dp', 'ep'))
    in_specs = (rows_spec,) * 3 + (P(),) * 11 + (P('ep'),) * 3
    return jax.shard_map(local, mesh=mesh, in_specs=in_specs, out_specs=rows_spec, check_vma=False)
```

```python
import functools

import jax
import jax.numpy as jnp
from jax import lax
from jax.experimental import pallas as pl
from jax.experimental.pallas import tpu as pltpu
from jax.sharding import PartitionSpec as P

HEAD = 128
EPS = 1e-6
ROPE_BASE = 10000.0
F32, BF = jnp.float32, jnp.bfloat16


def _rms(x, w):
    xf = x.astype(F32)
    r = lax.rsqrt(jnp.mean(xf * xf, axis=-1, keepdims=True) + EPS)
    return (xf * r * w.astype(F32).reshape(1, -1)).astype(BF)


def _dot(a, b):
    return jnp.dot(a, b, preferred_element_type=F32)


MESH = pl.DeviceIdType.MESH
MB = 128


def _peer(me, r):
    p = me
    if r & 1:
        p = p + 1 - 2 * (me % 2)
    if r & 2:
        p = p + 2 - 4 * ((me // 2) % 2)
    if r & 4:
        p = p + 4 - 8 * (me // 4)
    return p


def _barrier(me, rels):
    sem = pltpu.get_barrier_semaphore()
    for r in rels:
        pl.semaphore_signal(sem, inc=1, device_id={'ep': _peer(me, r)}, device_id_type=MESH)
    return lambda: pl.semaphore_wait(sem, len(rels))


def _rank(g):
    t = g.shape[1]
    before = jnp.where(lax.broadcasted_iota(jnp.int32, (t, t), 0) < lax.broadcasted_iota(jnp.int32, (t, t), 1), 1.0, 0.0)
    return jnp.where(g >= 0, _dot(jnp.where(g >= 0, 1.0, 0.0), before), -1.0)


class _Tiles:
    def __init__(self, hbm, vmem, sems, first, count):
        self.hbm, self.vmem, self.sems, self.first, self.count = hbm, vmem, sems, first, count

    def copies(self, k):
        slot = lax.rem(k, 2)
        ft = self.vmem[0].shape[-1]
        part = pl.ds(pl.multiple_of((self.first + k) * ft, ft), ft)
        w1, w3, w2 = self.hbm
        src = (w1.at[:, part], w3.at[:, part], w2.at[part])
        return [pltpu.make_async_copy(a, b.at[slot], c.at[slot]) for a, b, c in zip(src, self.vmem, self.sems)]

    def start(self, k):
        for c in self.copies(k):
            c.start()

    def add(self, k, z, acc_ref):
        for c in self.copies(k):
            c.wait()
        slot = lax.rem(k, 2)
        acc_ref[...] += _ffn_tile(z, *(v[slot] for v in self.vmem))

        @pl.when(k + 2 < self.count)
        def _():
            self.start(k + 2)


def _tile_scratch(d, ft):
    dma = pltpu.SemaphoreType.DMA
    return [pltpu.VMEM((2, d, ft), BF), pltpu.VMEM((2, d, ft), BF), pltpu.VMEM((2, ft, d), BF), dma((2,)), dma((2,)), dma((2,))]


def _ffn_tile(z, w1, w3, w2):
    h1 = _dot(z, w1)
    h3 = _dot(z, w3)
    hid = (h1 * jax.nn.sigmoid(h1) * h3).astype(BF)
    return _dot(hid, w2)


def _first_kernel(h_ref, na_ref, nm_ref, nf_ref, wr_ref, idx_ref, cos_ref, sin_ref, wq_ref, wk_ref, wv_ref, wo_ref,
                  w1_hbm, w3_hbm, w2_hbm, z_ref, f_ref, uall_ref, gall_ref, off_ref, gm_hbm,
                  x_sc, acc_sc, u_sc, g_sc, gv_sc, gm_sc, sa, ra, sb, rb, sc, rc, sg, rg, ls, lg, t1, t3, t2, q1, q3, q2s,
                  *, na_steps, nf_steps, hps, el, cap, step_b, step_c):
    i = pl.program_id(0)
    t, d = h_ref.shape
    me = lax.axis_index('ep')
    hops = (1, 2, 4)
    half = t // 2
    tiles = _Tiles((w1_hbm, w3_hbm, w2_hbm), (t1, t3, t2), (q1, q3, q2s), 0, nf_steps)

    def remote(src, dst, s, r, rel):
        return pltpu.make_async_remote_copy(src_ref=src, dst_ref=dst, send_sem=s, recv_sem=r,
                                            device_id={'ep': _peer(me, rel)}, device_id_type=MESH)

    sends_a = ((1, 0, t), (2, 0, half), (4, half, half), (2, half, half), (4, 0, half))

    def stage_a(n):
        rel, start, size = sends_a[n]
        rows = pl.ds(start, size)
        return remote(u_sc.at[rows], uall_ref.at[rel, rows], sa.at[n], ra.at[n], rel)

    def stage_g(r):
        rows = pl.ds(pl.multiple_of(_peer(me, r) * el, el), el)
        return remote(g_sc.at[rows], gv_sc.at[r], sg.at[r - 1], rg.at[r - 1], r)

    def stage_b(n):
        rows = pl.ds(n * half, half)
        return remote(uall_ref.at[(2, 4)[n], rows], uall_ref.at[6, rows], sb.at[n], rb.at[n], (4, 2)[n])

    def stage_c(n):
        return remote(uall_ref.at[2 * n + 2], uall_ref.at[2 * n + 3], sc.at[n], rc.at[n], 1)

    def own():
        return pltpu.make_async_copy(u_sc, uall_ref.at[0], ls.at[0])

    def put_g(r):
        return pltpu.make_async_copy(gm_sc.at[r % 2], gm_hbm.at[r], lg.at[r % 2])

    def combine_matrix(r):
        g = gv_sc[r]
        it = lax.broadcasted_iota(jnp.int32, (cap, t), 0).astype(F32)
        rank = _rank(g)
        gt = jnp.concatenate([jnp.where(it == rank[e:e + 1, :], g[e:e + 1, :], 0.0) for e in range(el)], axis=0)
        gm = jnp.transpose(gt)
        ghi = gm.astype(BF)
        r1 = gm - ghi.astype(F32)
        gmid = r1.astype(BF)
        glo = (r1 - gmid.astype(F32)).astype(BF)
        gm_sc[r % 2] = jnp.concatenate([ghi, gmid, glo], axis=1)

    @pl.when(i == 0)
    def _():
        arrived = _barrier(me, range(1, 8))
        u = _rms(h_ref[...], nm_ref[...])
        u_sc[...] = u
        logits = lax.dot_general(wr_ref[...], u, (((1,), (1,)), ((), ())), preferred_element_type=F32)
        row = lax.broadcasted_iota(jnp.int32, logits.shape, 0)
        routed = row == idx_ref[0:1, :]
        for j in range(1, idx_ref.shape[0]):
            routed = routed | (row == idx_ref[j:j + 1, :])
        lg = jnp.where(routed, logits, -jnp.inf)
        ex = jnp.exp(lg - jnp.max(lg, axis=0, keepdims=True))
        g_sc[...] = jnp.where(routed, ex / jnp.sum(ex, axis=0, keepdims=True), -1.0)
        arrived()
        for n in (1, 2, 3, 4, 0):
            stage_a(n).start()
        for r in range(1, 8):
            stage_g(r).start()
        own().start()
        gv_sc[0] = g_sc[pl.ds(pl.multiple_of(me * el, el), el), :]
        x_sc[...] = _rms(h_ref[...], na_ref[...])
        acc_sc[...] = jnp.zeros_like(acc_sc)

    for r in range(8):
        @pl.when(i == r + 1)
        def _():
            if r:
                stage_g(r).wait_recv()
            if r >= 2:
                put_g(r - 2).wait()
            combine_matrix(r)
            put_g(r).start()

    @pl.when(i < na_steps)
    def _():
        x = x_sc[...]
        q2 = _dot(x, wq_ref[...])
        k2 = _dot(x, wk_ref[...])
        v2 = _dot(x, wv_ref[...]).astype(BF)
        cos, sin = cos_ref[...], sin_ref[...]
        causal = lax.broadcasted_iota(jnp.int32, (t, t), 0) >= lax.broadcasted_iota(jnp.int32, (t, t), 1)
        outs = []
        for h in range(hps):
            sl = slice(h * HEAD, (h + 1) * HEAD)
            q, k, v = q2[:, sl], k2[:, sl], v2[:, sl]
            q = (q * cos + pltpu.roll(q, HEAD // 2, 1) * sin).astype(BF)
            k = (k * cos + pltpu.roll(k, HEAD // 2, 1) * sin).astype(BF)
            s = lax.dot_general(q, k, (((1,), (1,)), ((), ())), preferred_element_type=F32) * HEAD ** -0.5
            s = jnp.where(causal, s, -jnp.inf)
            p = jnp.exp(s - jnp.max(s, axis=-1, keepdims=True))
            p = (p / jnp.sum(p, axis=-1, keepdims=True)).astype(BF)
            outs.append(_dot(p, v).astype(BF))
        acc_sc[...] += _dot(jnp.concatenate(outs, axis=1), wo_ref[...])

    @pl.when(i == na_steps - 1)
    def _():
        a = (h_ref[...].astype(F32) + acc_sc[...]).astype(BF)
        f_ref[...] = a.astype(F32)
        z_ref[...] = _rms(a, nf_ref[...])

    @pl.when(i == step_b)
    def _():
        for n in range(2):
            stage_a(n + 1).wait_recv()
            stage_b(n).start()

    @pl.when(i == na_steps)
    def _():
        for n in range(2):
            stage_a(n + 3).wait_recv()
            stage_c(n).start()

    @pl.when(i == step_c)
    def _():
        for n in range(2):
            stage_b(n).wait_recv()
        stage_c(2).start()

    @pl.when(i == na_steps - 3)
    def _():
        tiles.start(0)
        tiles.start(1)

    @pl.when((i >= na_steps) & (i < na_steps + nf_steps))
    def _():
        tiles.add(i - na_steps, z_ref[...], f_ref)

    @pl.when(i == na_steps + nf_steps)
    def _():
        stage_a(0).wait_recv()
        for n in range(5):
            stage_a(n).wait_send()
        for n in range(2):
            stage_b(n).wait_send()
        for n in range(3):
            stage_c(n).wait()
        own().wait()
        for r in (6, 7):
            put_g(r).wait()

    @pl.when(i == na_steps + 1)
    def _():
        for r in range(1, 8):
            stage_g(r).wait_send()
        gall_ref[...] = gv_sc[...]
        base = jnp.zeros((el, 1), jnp.int32)
        for r in range(8):
            off_ref[r] = jnp.broadcast_to(base, (el, 128))
            cnt = jnp.sum(jnp.where(gv_sc[r] >= 0, 1.0, 0.0), axis=1, keepdims=True).astype(jnp.int32)
            base = base + (cnt + 15) // 16 * 16
        off_ref[8] = jnp.broadcast_to(jnp.maximum((base + MB - 1) // MB, 1), (el, 128))


def _first(h, na, nm, nf, wr, idx, wq, wk, wv, wo, w1, w3, w2, el, cap, nf_steps, ft):
    t, d = h.shape
    hps = 2
    w = HEAD * hps
    na_steps = wq.shape[1] // w
    ne = wr.shape[0]
    pos = jnp.arange(t).astype(F32)
    inv = ROPE_BASE ** (-2.0 * jnp.arange(HEAD // 2).astype(F32) / HEAD)
    ang = pos[:, None] * inv[None, :]
    c, s = jnp.cos(ang), jnp.sin(ang)
    cos, sin = jnp.concatenate([c, c], 1), jnp.concatenate([-s, s], 1)
    full = lambda shape: pl.BlockSpec(shape, lambda i: (0, 0))
    vec = pl.BlockSpec((d,), lambda i: (0,))
    ai = lambda i: jnp.minimum(i, na_steps - 1)
    any_ = pl.BlockSpec(memory_space=pl.ANY)
    dma = pltpu.SemaphoreType.DMA
    return pl.pallas_call(
        functools.partial(_first_kernel, na_steps=na_steps, nf_steps=nf_steps, hps=hps, el=el, cap=cap, step_b=na_steps - 2,
                          step_c=na_steps + nf_steps),
        grid=(na_steps + nf_steps + 1,),
        in_specs=[full((t, d)), vec, vec, vec, full((ne, d)), full(idx.shape),
                  full((t, HEAD)), full((t, HEAD))]
        + [pl.BlockSpec((d, w), lambda i: (0, ai(i)))] * 3
        + [pl.BlockSpec((w, d), lambda i: (ai(i), 0))]
        + [any_] * 3,
        out_specs=[full((t, d)), full((t, d)), any_, pl.BlockSpec((8, el, t), lambda i: (0, 0, 0)),
                   pl.BlockSpec((9, el, 128), lambda i: (0, 0, 0)), any_],
        out_shape=[jax.ShapeDtypeStruct((t, d), BF), jax.ShapeDtypeStruct((t, d), F32),
                   jax.ShapeDtypeStruct((8, t, d), BF), jax.ShapeDtypeStruct((8, el, t), F32),
                   jax.ShapeDtypeStruct((9, el, 128), jnp.int32), jax.ShapeDtypeStruct((8, t, 3 * el * cap), BF)],
        scratch_shapes=[pltpu.VMEM((t, d), BF), pltpu.VMEM((t, d), F32), pltpu.VMEM((t, d), BF),
                        pltpu.VMEM((ne, t), F32), pltpu.VMEM((8, el, t), F32), pltpu.VMEM((2, t, 3 * el * cap), BF),
                        dma((5,)), dma((5,)), dma((2,)), dma((2,)), dma((3,)), dma((3,)), dma((7,)), dma((7,)), dma((1,)), dma((2,))] + _tile_scratch(d, ft),
        cost_estimate=pl.CostEstimate(flops=8 * t * d * d, bytes_accessed=8 * d * d, transcendentals=0),
        compiler_params=pltpu.CompilerParams(dimension_semantics=("arbitrary",), collective_id=0, has_side_effects=True,
                                             vmem_limit_bytes=56 << 20),
        name="first",
    )(h, na, nm, nf, wr, idx, cos, sin, wq, wk, wv, wo, w1, w3, w2)


def _hid_kernel(off_ref, g_ref, u_hbm, w1_hbm, w3_hbm, hid_hbm,
                u_sc, x_sc, w1_sc, w3_sc, h_sc, hx_sc, su, sw1, sw3, sh, *, ns, el, cap, nf, mb, depth):
    t, d = u_sc.shape[1:]
    ft = w1_sc.shape[-1]
    rows = ns * cap
    total = el * nf

    def fetch(k):
        slot = lax.rem(k, depth)
        e, f = lax.div(k, nf), lax.rem(k, nf)
        cols = pl.ds(pl.multiple_of(f * ft, ft), ft)
        return (pltpu.make_async_copy(w1_hbm.at[e, :, cols], w1_sc.at[slot], sw1.at[slot]),
                pltpu.make_async_copy(w3_hbm.at[e, :, cols], w3_sc.at[slot], sw3.at[slot]))

    def put_h(k):
        slot = lax.rem(k, 2)
        e, f = lax.div(k, nf), lax.rem(k, nf)
        cols = pl.ds(pl.multiple_of(f * ft, ft), ft)
        return pltpu.make_async_copy(hx_sc.at[slot], hid_hbm.at[e, :, cols], sh.at[slot])

    def get_u(s):
        return pltpu.make_async_copy(u_hbm.at[s], u_sc.at[s], su.at[s])

    for s in range(ns):
        get_u(s).start()
    for k in range(depth):
        for c in fetch(k):
            c.start()
    h_sc[...] = jnp.zeros_like(h_sc)
    it = lax.broadcasted_iota(jnp.int32, (cap, t), 0).astype(F32)

    @pl.loop(0, ns)
    def _(s):
        rank = _rank(g_ref[s])
        p = jnp.concatenate([jnp.where(it == rank[e:e + 1, :], 1.0, 0.0).astype(BF) for e in range(el)], axis=0)
        get_u(s).wait()
        for c in range(d // 512):
            cs = slice(c * 512, (c + 1) * 512)
            xv = _dot(p, u_sc[s, :, cs]).astype(BF)
            for e in range(el):
                o = pl.multiple_of(off_ref[s, e, 0], 16)
                x_sc[e, pl.ds(o, cap), cs] = xv[e * cap:(e + 1) * cap]

    @pl.loop(0, total)
    def _(k):
        slot = lax.rem(k, depth)
        e = lax.div(k, nf)
        for c in fetch(k):
            c.wait()
        for m in range(mb, rows + 1, mb):
            @pl.when(off_ref[ns, e, 0] == m // mb)
            def _():
                x = x_sc[e, :m, :]
                h1 = _dot(x, w1_sc[slot])
                h3 = _dot(x, w3_sc[slot])
                h_sc[:m, :] = (h1 * jax.nn.sigmoid(h1) * h3).astype(BF)

        @pl.when(k + depth < total)
        def _():
            for c in fetch(k + depth):
                c.start()

        @pl.when(k >= 2)
        def _():
            put_h(k - 2).wait()
        for s in range(ns):
            o = pl.multiple_of(off_ref[s, e, 0], 16)
            hx_sc[lax.rem(k, 2), s * cap:(s + 1) * cap, :] = h_sc[pl.ds(o, cap), :]
        put_h(k).start()

    for k in (total - 2, total - 1):
        put_h(k).wait()


def _hidden(u_all, g_all, off, ue1, ue3, cap):
    ns, t, d = u_all.shape
    el, _, fe = ue1.shape
    mb, nf, depth = MB, 2, 4
    ft = fe // nf
    smem, vmem, any_ = (pl.BlockSpec(memory_space=m) for m in (pltpu.SMEM, pltpu.VMEM, pl.ANY))
    dma = pltpu.SemaphoreType.DMA
    return pl.pallas_call(
        functools.partial(_hid_kernel, ns=ns, el=el, cap=cap, nf=nf, mb=mb, depth=depth),
        in_specs=[smem, vmem, any_, any_, any_],
        out_specs=any_,
        out_shape=jax.ShapeDtypeStruct((el, ns * cap, fe), BF),
        scratch_shapes=[pltpu.VMEM((ns, t, d), BF), pltpu.VMEM((el, ns * cap, d), BF), pltpu.VMEM((depth, d, ft), BF),
                        pltpu.VMEM((depth, d, ft), BF), pltpu.VMEM((ns * cap, ft), BF), pltpu.VMEM((2, ns * cap, ft), BF),
                        dma((ns,)), dma((depth,)), dma((depth,)), dma((2,))],
        cost_estimate=pl.CostEstimate(flops=4 * el * ns * cap * d * fe, bytes_accessed=4 * el * d * fe, transcendentals=0),
        compiler_params=pltpu.CompilerParams(vmem_limit_bytes=58 << 20),
        name="hidden",
    )(off, g_all, u_all, ue1, ue3)


E0 = {q: q + 1 for q in range(8)}
E1 = {0: 2, 1: 3, 2: 5, 3: 6, 4: 7, 5: 9, 6: 12, 7: 15}
E2 = {0: 8, 1: 8, 2: 11, 3: 12, 4: 14, 5: 16, 6: 16, 7: 16}
NQ, F_FROM, STEPS = 8, 4, 17


def _last_kernel(hid_hbm, gm_hbm, z_hbm, f_hbm, ue2_ref, w1_hbm, w3_hbm, w2_hbm, o_ref,
                 hid_sc, gm_sc, z_ref, y_sc, keep_sc, ps_sc, r0_sc, r1_sc, r2_sc, acc_sc, hs, gs, zs, s0, r0, s1, r1, s2, r2,
                 t1, t3, t2, q1, q3, q2s, *, ns, el, cap, f0, nfs):
    i = pl.program_id(0)
    t, d = z_ref.shape
    half = t // 2
    cw = ue2_ref.shape[-1]
    me = lax.axis_index('ep')
    tiles = _Tiles((w1_hbm, w3_hbm, w2_hbm), (t1, t3, t2), (q1, q3, q2s), f0, nfs)

    def get_h(e):
        return pltpu.make_async_copy(hid_hbm.at[e], hid_sc.at[e], hs.at[e])

    def get_g(s):
        return pltpu.make_async_copy(gm_hbm.at[s], gm_sc.at[s], gs.at[s])

    def remote(src, dst, s, r, dev):
        return pltpu.make_async_remote_copy(src_ref=src, dst_ref=dst, send_sem=s, recv_sem=r,
                                            device_id={'ep': dev}, device_id_type=MESH)

    def get_zf():
        return (pltpu.make_async_copy(z_hbm, z_ref, zs.at[0]), pltpu.make_async_copy(f_hbm, acc_sc, zs.at[1]))

    def send0(q, slot):
        return remote(ps_sc.at[slot], r0_sc.at[q], s0.at[q], r0.at[q], _peer(me, 1))

    def send1(q, h):
        return remote(r0_sc.at[q, h, pl.ds(2, 2)], r1_sc.at[q, h], s1.at[2 * q + h], r1.at[2 * q + h], _peer(me, (2, 4)[h]))

    def send2(q, h):
        return remote(r0_sc.at[q, h, 1], r2_sc.at[q, h], s2.at[2 * q + h], r2.at[2 * q + h], _peer(me, (4, 2)[h]))

    @pl.when(i == 0)
    def _():
        arrived = _barrier(me, (1, 2, 4))
        for e in range(el):
            get_h(e).start()
        for s in range(ns):
            get_g(s).start()
        for c in get_zf():
            c.start()
        arrived()

    def pass_on(qs):
        for q in qs:
            @pl.when(i == E0[q])
            def _():
                send0(q, q % 2).wait_recv()
                r0_sc[q] += keep_sc[...]
                for h in range(2):
                    send1(q, h).start()

    pass_on((0, 1))

    def expert(e):
        y = _dot(hid_sc[e], ue2_ref[e]).astype(BF)
        for s in range(ns):
            y_sc[s, e * cap:(e + 1) * cap, :] = y[s * cap:(s + 1) * cap]

    @pl.when(i == 0)
    def _():
        for e in range(el):
            get_h(e).wait()
            expert(e)

    @pl.when((i > 0) & (i < NQ))
    def _():
        for e in range(el):
            expert(e)

    pass_on(range(2, NQ))

    @pl.when(i == 0)
    def _():
        for s in range(ns):
            get_g(s).wait()
        tiles.start(0)
        tiles.start(1)

    @pl.when((i >= 2) & (i < NQ))
    def _():
        send0(i - 2, i % 2).wait_send()

    @pl.when(i < NQ)
    def _():
        kk = el * cap
        for c in (1, 0):
            for b in range(4):
                s = 2 * b + c
                y = y_sc[s]
                m = _dot(gm_sc[s, :, :kk], y) + _dot(gm_sc[s, :, kk:2 * kk], y) + _dot(gm_sc[s, :, 2 * kk:], y)
                for h, pos in enumerate(((0, 2, 1, 3)[b], b)):
                    part = m[h * half:(h + 1) * half]
                    if c == 0:
                        keep_sc[h, pos] = part
                    else:
                        ps_sc[i % 2, h, pos] = part
            if c == 1:
                send0(i, i % 2).start()

    @pl.when(i == F_FROM)
    def _():
        for c in get_zf():
            c.wait()

    @pl.when((i >= F_FROM) & (i < F_FROM + nfs))
    def _():
        tiles.add(i - F_FROM, z_ref[...], acc_sc)

    for q, step in E1.items():
        @pl.when(i == step)
        def _():
            for h in range(2):
                send1(q, h).wait_recv()
                r0_sc[q, h, 0:2] += r1_sc[q, h]
                send2(q, h).start()

    for q, step in E2.items():
        @pl.when(i == step)
        def _():
            for h in range(2):
                send2(q, h).wait_recv()
                acc_sc[h * half:(h + 1) * half, q * cw:(q + 1) * cw] += r0_sc[q, h, 0] + r2_sc[q, h]

    @pl.when(i == STEPS - 1)
    def _():
        for q in (NQ - 2, NQ - 1):
            send0(q, q % 2).wait_send()
        for q in range(NQ):
            for h in range(2):
                send1(q, h).wait_send()
                send2(q, h).wait_send()
        o_ref[...] = acc_sc[...].astype(BF)


def _last(hid, gm, z, f, ue2, w1, w3, w2, cap, ft, f0):
    t, d = z.shape
    el, rows, fe = hid.shape
    ns = rows // cap
    cw = d // NQ
    nfs = w1.shape[1] // ft - f0
    full = lambda shape: pl.BlockSpec(shape, lambda i: (0, 0), pipeline_mode=pl.Buffered(1))
    qi = lambda i: jnp.minimum(i, NQ - 1)
    any_ = pl.BlockSpec(memory_space=pl.ANY)
    dma = pltpu.SemaphoreType.DMA
    return pl.pallas_call(
        functools.partial(_last_kernel, ns=ns, el=el, cap=cap, f0=f0, nfs=nfs),
        grid=(STEPS,),
        in_specs=[any_, any_, any_, any_,
                  pl.BlockSpec((el, fe, cw), lambda i: (0, 0, qi(i)))] + [any_] * 3,
        out_specs=full((t, d)),
        out_shape=jax.ShapeDtypeStruct((t, d), BF),
        scratch_shapes=[pltpu.VMEM((el, rows, fe), BF), pltpu.VMEM(gm.shape, BF), pltpu.VMEM((t, d), BF),
                        pltpu.VMEM((ns, el * cap, cw), BF),
                        pltpu.VMEM((2, 4, t // 2, cw), F32), pltpu.VMEM((2, 2, 4, t // 2, cw), F32),
                        pltpu.VMEM((NQ, 2, 4, t // 2, cw), F32), pltpu.VMEM((NQ, 2, 2, t // 2, cw), F32),
                        pltpu.VMEM((NQ, 2, t // 2, cw), F32), pltpu.VMEM((t, d), F32),
                        dma((el,)), dma((ns,)), dma((2,))] + [dma((NQ,))] * 2 + [dma((2 * NQ,))] * 4 + _tile_scratch(d, ft),
        cost_estimate=pl.CostEstimate(flops=2 * el * rows * d * fe, bytes_accessed=2 * el * d * fe, transcendentals=0),
        compiler_params=pltpu.CompilerParams(dimension_semantics=("arbitrary",), collective_id=1, has_side_effects=True,
                                             vmem_limit_bytes=67043328),
        name="last",
    )(hid, gm, z, f, ue2, w1, w3, w2)


def solution(mesh):
    G = mesh.shape['ep']
    ft, f0 = 512, 4

    def local(h0, idx, slot, na, wq, wk, wv, wo, nf, w1, w3, w2, nm, wr, ue1, ue3, ue2):
        b, s, d = h0.shape
        t = b * s
        k = idx.shape[-1]
        el = ue1.shape[0]
        cap = 2 * t * k // (el * G)
        z, f, u_all, g_all, off, gm = _first(h0.reshape(t, d), na, nm, nf, wr.T, idx.reshape(t, k).T, wq, wk, wv, wo, w1, w3, w2,
                                         el, cap, f0, ft)
        hid = _hidden(u_all, g_all, off, ue1, ue3, cap)
        return _last(hid, gm, z, f, ue2, w1, w3, w2, cap, ft, f0).reshape(b, s, d)

    rows_spec = P(('dp', 'ep'))
    in_specs = (rows_spec,) * 3 + (P(),) * 11 + (P('ep'),) * 3
    return jax.shard_map(local, mesh=mesh, in_specs=in_specs, out_specs=rows_spec, check_vma=False)
```
